32 devices in a mesh: dp: 1 (over z), dm: 4 (over y), tp: 8 (over x, core).
Axes of the slice: x: 4, y: 4, z: 1, core: 2. Of those that a mesh axis runs over, the one named last changes fastest.
The devices are a block of a 4x4x8 slice.
Arguments:
- hidden: bfloat16 [256, 5120], P('dp', 'dm')
- w_q: bfloat16 [5120, 40, 128], P('dm', 'tp')
- w_k: bfloat16 [5120, 40, 128], P('dm', 'tp')
- w_v: bfloat16 [5120, 40, 128], P('dm', 'tp')
- w_o: bfloat16 [40, 128, 5120], P('tp', None, 'dm')
- w_gate: bfloat16 [5120, 13824], P('dm', 'tp')
- w_up: bfloat16 [5120, 13824], P('dm', 'tp')
- w_down: bfloat16 [13824, 5120], P('tp', 'dm')
- norm_attn: bfloat16 [5120], P('dm')
- norm_mlp: bfloat16 [5120], P('dm')
- k_cache: bfloat16 [256, 64, 40, 128], P(('dp', 'dm'), None, 'tp')
- v_cache: bfloat16 [256, 64, 40, 128], P(('dp', 'dm'), None, 'tp')
- seq_lens: int32 [256], P(('dp', 'dm'))
- rope_cos: float32 [256, 64], P(('dp', 'dm'))
- rope_sin: float32 [256, 64], P(('dp', 'dm'))
Outputs:
- output 1: bfloat16 [256, 5120], P('dp', 'dm')
- output 2: bfloat16 [256, 64, 40, 128], P(('dp', 'dm'), None, 'tp')
- output 3: bfloat16 [256, 64, 40, 128], P(('dp', 'dm'), None, 'tp')
All inputs are finite; a program needn't handle non-finite values.
Results may differ from the reference program's by a relative error of at most 0.0106647.
Values are sent between devices in bfloat16 or wider.
A program may use at most 768 MiB of HBM per device.

```python
import math
import jax
import jax.numpy as jnp
from jax import lax

D = 5120
HEADS = 40
KV_HEADS = 40
HEAD = 128
FF = 13824
BATCH = 256
SEQ = 64

GROUP = HEADS // KV_HEADS
HALF = HEAD // 2
EPS = 1e-6
ROPE_BASE = 10000.0
K_SCALE = math.sqrt(max(math.log(SEQ / 16.0), 1.0))


def rope_tables(seq_lens):
    inv_freq = ROPE_BASE ** (-2.0 * jnp.arange(HALF, dtype=jnp.float32) / HEAD)
    angles = seq_lens.astype(jnp.float32)[:, None] * inv_freq[None, :]
    return jnp.cos(angles), jnp.sin(angles)


def draw_lengths(key):
    lengths = jax.random.randint(key, (BATCH,), SEQ // 8, SEQ, dtype=jnp.int32)
    return lengths.at[0].set(SEQ - 1).at[BATCH - 1].set(SEQ // 8)


def setup_inputs(seed: int = 0, part: int = 0) -> dict:
    shared = jax.random.split(jax.random.key(seed), 9)
    local = jax.random.split(jax.random.fold_in(jax.random.key(seed), part), 4)
    w_q = (jax.random.normal(shared[0], (D, HEADS, HEAD), jnp.float32) * D ** -0.5).astype(jnp.bfloat16)
    w_k = (jax.random.normal(shared[1], (D, KV_HEADS, HEAD), jnp.float32) * (K_SCALE * D ** -0.5)).astype(jnp.bfloat16)
    w_v = (jax.random.normal(shared[2], (D, KV_HEADS, HEAD), jnp.float32) * D ** -0.5).astype(jnp.bfloat16)
    w_o = (jax.random.normal(shared[3], (HEADS, HEAD, D), jnp.float32) * (HEADS * HEAD) ** -0.5).astype(jnp.bfloat16)
    w_gate = (jax.random.normal(shared[4], (D, FF), jnp.float32) * D ** -0.5).astype(jnp.bfloat16)
    w_up = (jax.random.normal(shared[5], (D, FF), jnp.float32) * D ** -0.5).astype(jnp.bfloat16)
    w_down = (jax.random.normal(shared[6], (FF, D), jnp.float32) * FF ** -0.5).astype(jnp.bfloat16)
    norm_attn = (1.0 + 0.4 * jax.random.normal(shared[7], (D,), jnp.float32)).astype(jnp.bfloat16)
    norm_mlp = (1.0 + 0.4 * jax.random.normal(shared[8], (D,), jnp.float32)).astype(jnp.bfloat16)
    hidden = jax.random.normal(local[0], (BATCH, D), jnp.float32).astype(jnp.bfloat16)
    k_cache = (jax.random.normal(local[1], (BATCH, SEQ, KV_HEADS, HEAD), jnp.float32) * K_SCALE).astype(jnp.bfloat16)
    v_cache = jax.random.normal(local[2], (BATCH, SEQ, KV_HEADS, HEAD), jnp.float32).astype(jnp.bfloat16)
    seq_lens = draw_lengths(local[3])
    rope_cos, rope_sin = rope_tables(seq_lens)
    return dict(hidden=hidden, w_q=w_q, w_k=w_k, w_v=w_v, w_o=w_o, w_gate=w_gate, w_up=w_up, w_down=w_down, norm_attn=norm_attn, norm_mlp=norm_mlp, k_cache=k_cache, v_cache=v_cache, seq_lens=seq_lens, rope_cos=rope_cos, rope_sin=rope_sin)


def rms_norm(x, gain):
    x_f32 = x.astype(jnp.float32)
    scale = lax.rsqrt(jnp.mean(x_f32 * x_f32, axis=-1, keepdims=True) + EPS)
    return (x_f32 * scale * gain.astype(jnp.float32)).astype(jnp.bfloat16)


def apply_rope(x, rope_cos, rope_sin):
    first = x[..., :HALF]
    second = x[..., HALF:]
    cosine = rope_cos[:, None, :]
    sine = rope_sin[:, None, :]
    return jnp.concatenate([first * cosine - second * sine, second * cosine + first * sine], axis=-1).astype(jnp.bfloat16)


def project(x, weight):
    return jnp.dot(x, weight.reshape(D, -1), preferred_element_type=jnp.float32).reshape(BATCH, -1, HEAD)


def attend_row(row_args):
    q_row, k_row, v_row, length = row_args
    q_grp = q_row.reshape(KV_HEADS, GROUP, HEAD).astype(jnp.float32)
    scores = jnp.einsum('kgd,skd->kgs', q_grp, k_row.astype(jnp.float32)) / math.sqrt(HEAD)
    key_mask = jnp.arange(SEQ)[None, None, :] <= length
    scores = jnp.where(key_mask, scores, -1e30)
    attn_probs = jax.nn.softmax(scores, axis=-1).astype(jnp.bfloat16).astype(jnp.float32)
    heads = jnp.einsum('kgs,skd->kgd', attn_probs, v_row.astype(jnp.float32))
    return heads.reshape(HEADS, HEAD).astype(jnp.bfloat16)


def reference(hidden, w_q, w_k, w_v, w_o, w_gate, w_up, w_down, norm_attn, norm_mlp, k_cache, v_cache, seq_lens, rope_cos, rope_sin):
    x_norm = rms_norm(hidden, norm_attn)
    q_rot = apply_rope(project(x_norm, w_q), rope_cos, rope_sin)
    k_rot = apply_rope(project(x_norm, w_k), rope_cos, rope_sin)
    v_new = project(x_norm, w_v).astype(jnp.bfloat16)
    write_mask = (jnp.arange(SEQ)[None, :] == seq_lens[:, None])[:, :, None, None]
    k_out = jnp.where(write_mask, k_rot[:, None], k_cache)
    v_out = jnp.where(write_mask, v_new[:, None], v_cache)
    attn_heads = lax.map(attend_row, (q_rot, k_out, v_out, seq_lens))
    attn_out = jnp.dot(attn_heads.reshape(BATCH, HEADS * HEAD), w_o.reshape(HEADS * HEAD, D), preferred_element_type=jnp.float32).astype(jnp.bfloat16)
    h_mid = hidden + attn_out
    x_mlp = rms_norm(h_mid, norm_mlp)
    gate = jnp.dot(x_mlp, w_gate, preferred_element_type=jnp.float32)
    up_proj = jnp.dot(x_mlp, w_up, preferred_element_type=jnp.float32)
    gated_act = (jax.nn.silu(gate) * up_proj).astype(jnp.bfloat16)
    mlp_out = jnp.dot(gated_act, w_down, preferred_element_type=jnp.float32).astype(jnp.bfloat16)
    return (h_mid + mlp_out, k_out, v_out)
```

```python
import functools

import jax
import jax.numpy as jnp
from jax import lax
from jax.experimental import pallas as pl
from jax.experimental.pallas import tpu as pltpu
from jax.sharding import PartitionSpec as P

EPS = 1e-6
F32 = jnp.float32
BF16 = jnp.bfloat16
MESH = pl.DeviceIdType.MESH
PARTS = 3


def remote(src, dst, send, recv, axis, index):
    return pltpu.make_async_remote_copy(
        src_ref=src, dst_ref=dst, send_sem=send, recv_sem=recv, device_id={axis: index}, device_id_type=MESH)


def entry_barrier(peers):
    barrier = pltpu.get_barrier_semaphore()
    for axis, index in peers:
        pl.semaphore_signal(barrier, inc=1, device_id={axis: index}, device_id_type=MESH)
    return lambda: pl.semaphore_wait(barrier, len(peers))


def column_to_row(col):
    rows = col.shape[0]
    return jnp.concatenate(
        [jnp.broadcast_to(col[i:i + 128], (128, 128)).T[:8] for i in range(0, rows, 128)], axis=1)


def row_to_column(row):
    rows = row.shape[1]
    return jnp.concatenate(
        [jnp.broadcast_to(row[:1, i:i + 128], (128, 128)).T for i in range(0, rows, 128)], axis=0)


def scale_rows(x, scale, gain):
    width = x.shape[1]
    cols = [x[:, i:i + 128] * scale * gain[:, i:i + 128] for i in range(0, width, 128)]
    return jnp.concatenate(cols, axis=1).astype(BF16)


def qkv_kernel(nd, width_full, h_ref, g_ref, cos_ref, sin_ref, wq_hbm, wk_hbm, wv_hbm, q_out, k_out, v_out,
               w_buf, x_buf, part, ss_send, ss_recv, a_recv, b_recv, c_send, c_recv, cos2, sin2,
               w_sem, ss_s, ss_r, a_s, a_r, b_s, b_r, c_s, c_r):
    dm = lax.axis_index('dm')
    nxt, prv, far = lax.rem(dm + 1, nd), lax.rem(dm + nd - 1, nd), lax.rem(dm + 2, nd)
    rows = h_ref.shape[0] // nd
    half = rows // 2
    heads = w_buf.shape[1]

    wait_barrier = entry_barrier([('dm', nxt), ('dm', prv), ('dm', far)])
    loads = [pltpu.make_async_copy(src, w_buf.at[t], w_sem.at[t]) for t, src in enumerate((wq_hbm, wk_hbm, wv_hbm))]
    for load in loads:
        load.start()

    x = h_ref[...].astype(F32)
    ss_send[...] = column_to_row(jnp.sum(x * x, axis=-1, keepdims=True))
    wait_barrier()
    ss = [remote(ss_send, ss_recv.at[i], ss_s.at[i], ss_r.at[i], 'dm', peer) for i, peer in enumerate((nxt, prv, far))]
    for copy in ss:
        copy.start()
    hd = cos_ref.shape[1]
    cos2[:, :hd] = cos_ref[...]
    cos2[:, hd:] = cos_ref[...]
    sin2[:, :hd] = -sin_ref[...]
    sin2[:, hd:] = sin_ref[...]
    for copy in ss:
        copy.wait_recv()
    total = ss_send[...] + ss_recv[0] + ss_recv[1] + ss_recv[2]
    scale = row_to_column(lax.rsqrt(total / width_full + EPS))
    x_buf[...] = scale_rows(h_ref[...].astype(F32), scale, g_ref[...].astype(F32))

    def block(owner, second):
        return pl.ds(pl.multiple_of(owner * rows + second * half, half), half)

    peers = (nxt, prv)
    sends = []
    for t in range(3):
        loads[t].wait()
        for hh in range(heads):
            part[t, :, hh * 128:(hh + 1) * 128] = jnp.dot(x_buf[...], w_buf[t, hh], preferred_element_type=F32)
        for d in range(2):
            sends.append(remote(part.at[t, block(far, d)], a_recv.at[d, t], a_s.at[d, t], a_r.at[d, t], 'dm', peers[d]))
            sends[-1].start()
        for d in range(2):
            sends.append(remote(part.at[t, block(peers[d], 1 - d)], b_recv.at[d, t], b_s.at[d, t], b_r.at[d, t], 'dm', peers[d]))
            sends[-1].start()
    for t in range(3):
        for d in range(2):
            remote(a_recv.at[d, t], a_recv.at[d, t], a_s.at[d, t], a_r.at[d, t], 'dm', peers[d]).wait_recv()
            c_send[d, t] = a_recv[d, t] + part[t, block(peers[d], d)]
            sends.append(remote(c_send.at[d, t], c_recv.at[d, t], c_s.at[d, t], c_r.at[d, t], 'dm', peers[d]))
            sends[-1].start()
    for t, out in enumerate((q_out, k_out, v_out)):
        for d in range(2):
            remote(b_recv.at[d, t], b_recv.at[d, t], b_s.at[d, t], b_r.at[d, t], 'dm', peers[d]).wait_recv()
            remote(c_recv.at[d, t], c_recv.at[d, t], c_s.at[d, t], c_r.at[d, t], 'dm', peers[d]).wait_recv()
        for d in range(2):
            tot = part[t, block(dm, d)] + c_recv[d, t] + b_recv[1 - d, t]
            for hh in range(heads):
                y = tot[:, hh * 128:(hh + 1) * 128]
                if t < 2:
                    here = slice(d * half, (d + 1) * half)
                    y = y * cos2[here] + pltpu.roll(y, 64, 1) * sin2[here]
                out[d * half:(d + 1) * half, hh * 128:(hh + 1) * 128] = y.astype(BF16).astype(F32)
    for copy in ss + sends:
        copy.wait_send()


def qkv(nd, hidden, g, cos, sin, wq, wk, wv):
    batch, width = hidden.shape
    heads, _, head = wq.shape
    rows, cols = batch // nd, heads * head
    half = rows // 2
    vmem = pl.BlockSpec(memory_space=pltpu.VMEM)
    hbm = pl.BlockSpec(memory_space=pl.ANY)
    dma = pltpu.SemaphoreType.DMA
    piece = pltpu.VMEM((2, 3, half, cols), F32)
    return pl.pallas_call(
        functools.partial(qkv_kernel, nd, width * nd),
        out_shape=[jax.ShapeDtypeStruct((rows, cols), F32)] * 3,
        in_specs=[vmem] * 4 + [hbm] * 3,
        out_specs=[vmem] * 3,
        scratch_shapes=[
            pltpu.VMEM((3, heads, width, head), BF16), pltpu.VMEM((batch, width), BF16), pltpu.VMEM((3, batch, cols), F32),
            pltpu.VMEM((8, batch), F32), pltpu.VMEM((3, 8, batch), F32), piece, piece, piece, piece,
            pltpu.VMEM((rows, head), F32), pltpu.VMEM((rows, head), F32),
            dma((3,)), dma((3,)), dma((3,))] + [dma((2, 3))] * 6,
        compiler_params=pltpu.CompilerParams(collective_id=0, has_side_effects=True, vmem_limit_bytes=40 * 2 ** 20),
        name='qkv',
    )(hidden, g, cos, sin, wq, wk, wv)


def attend_kernel(lens_ref, q_ref, kn_ref, vn_ref, kc_ref, vc_ref, ko_ref, vo_ref, o_ref):
    step = pl.program_id(0)
    rb, heads, slots, head = kc_ref.shape
    pos = lax.broadcasted_iota(jnp.int32, (heads, slots, head), 1)
    head_row = lax.broadcasted_iota(jnp.int32, (8, heads * slots), 0)
    lane = lax.broadcasted_iota(jnp.int32, (8, heads * slots), 1)
    lane_slot = lane % slots
    own_head = (lane // slots) == head_row
    q_row = lax.broadcasted_iota(jnp.int32, (8, head), 0)
    q_all, kn_all, vn_all = q_ref[...], kn_ref[...], vn_ref[...]
    for r in range(rb):
        length = lens_ref[step * rb + r]
        write = pos == length

        def new(vals):
            return jnp.stack([jnp.broadcast_to(vals[r:r + 1, i * head:(i + 1) * head], (slots, head)) for i in range(heads)])

        k = jnp.where(write, new(kn_all), kc_ref[r].astype(F32)).astype(BF16)
        v = jnp.where(write, new(vn_all), vc_ref[r].astype(F32)).astype(BF16)
        ko_ref[r] = k
        vo_ref[r] = v
        q = jnp.zeros((8, head), F32)
        for i in range(heads):
            q = jnp.where(q_row == i, jnp.broadcast_to(q_all[r:r + 1, i * head:(i + 1) * head], (8, head)), q)
        s = lax.dot_general(q.astype(BF16), k.reshape(heads * slots, head), (((1,), (1,)), ((), ())), preferred_element_type=F32)
        s = jnp.where(own_head & (lane_slot <= length), s * (head ** -0.5), float(jnp.finfo(F32).min))
        p = jnp.exp(s - jnp.max(s, axis=-1, keepdims=True))
        p = jnp.where(own_head & (lane_slot <= length), p, 0.0)
        p = (p / jnp.maximum(jnp.sum(p, axis=-1, keepdims=True), 1e-30)).astype(BF16)
        o = jnp.dot(p, v.reshape(heads * slots, head), preferred_element_type=F32)
        for i in range(heads):
            o_ref[r:r + 1, i * head:(i + 1) * head] = o[i:i + 1]


def attend(lens, q, kn, vn, kc, vc):
    rows, heads, slots, head = kc.shape
    rb = 8
    row_block = pl.BlockSpec((rb, heads * head), lambda i, lens: (i, 0))
    cache_block = pl.BlockSpec((rb, heads, slots, head), lambda i, lens: (i, 0, 0, 0))
    return pl.pallas_call(
        attend_kernel,
        grid_spec=pltpu.PrefetchScalarGridSpec(
            num_scalar_prefetch=1, grid=(rows // rb,),
            in_specs=[row_block] * 3 + [cache_block] * 2,
            out_specs=[cache_block, cache_block, row_block]),
        out_shape=[jax.ShapeDtypeStruct(kc.shape, BF16), jax.ShapeDtypeStruct(vc.shape, BF16),
                   jax.ShapeDtypeStruct((rows, heads * head), F32)],
        compiler_params=pltpu.CompilerParams(vmem_limit_bytes=40 * 2 ** 20),
        name='attend',
    )(lens, q, kn, vn, kc, vc)


def mlp_kernel(nd, nx, width_full, o_ref, h_ref, g_ref, wo_hbm, wg_hbm, wu_hbm, wd_hbm, out_ref,
               wo, wg, wu, wd, o_all, part, d2d_recv, xa_recv, xb_recv, xc_send, xc_recv, h1_buf, ss_send, ss_recv,
               x2_all, gu, ga_recv, gb_recv, gc_send, gc_recv, m_all, h_all,
               w_sem, o_s, o_r, d_s, d_r, xa_s, xa_r, xb_s, xb_r, xc_s, xc_r, ss_s, ss_r,
               ag_s, ag_r, agf_s, agf_r, agd_s, agd_r, ga_s, ga_r, gb_s, gb_r, gc_s, gc_r, m_s, m_r, mf_s, mf_r):
    dm, tp = lax.axis_index('dm'), lax.axis_index('tp')
    nxt, prv, far = lax.rem(dm + 1, nd), lax.rem(dm + nd - 1, nd), lax.rem(dm + 2, nd)
    core, xi = lax.rem(tp, 2), tp // 2
    xn, xp, xf = lax.rem(xi + 1, nx), lax.rem(xi + nx - 1, nx), lax.rem(xi + 2, nx)
    partner = tp + 1 - 2 * core
    ypeers, xpeers, xpeer_ids = (nxt, prv), (xn, xp), (2 * xn + core, 2 * xp + core)
    batch, width = h_ref.shape
    rows = batch // nd
    share = batch // (2 * nx)
    xhalf = share // 2
    cols = wd.shape[0]
    own_cols = cols // nd
    pc = own_cols // PARTS
    ph = pc // 2
    sends = []

    def go(*args):
        sends.append(remote(*args))
        sends[-1].start()

    def got(ref, send, recv, axis, index):
        remote(ref, ref, send, recv, axis, index).wait_recv()

    wait_barrier = entry_barrier([('dm', nxt), ('dm', prv), ('dm', far), ('tp', partner), ('tp', xpeer_ids[0]), ('tp', xpeer_ids[1])])
    loads = [pltpu.make_async_copy(src, dst, w_sem.at[i])
             for i, (src, dst) in enumerate(((wo_hbm, wo), (wg_hbm, wg), (wu_hbm, wu), (wd_hbm, wd)))]
    for load in loads:
        load.start()

    def rows_of(owner, offset=0, count=rows):
        return pl.ds(pl.multiple_of(owner * rows + offset, 16), count)

    o_all[rows_of(dm)] = o_ref[...].astype(BF16)
    wait_barrier()
    for d in range(2):
        mine = o_all.at[rows_of(dm)]
        go(mine, mine, o_s.at[0, d], o_r.at[0, d], 'dm', ypeers[d])
    for d in range(2):
        near = o_all.at[rows_of(ypeers[1 - d])]
        got(near, o_s.at[0, d], o_r.at[0, d], 'dm', ypeers[d])
        piece = o_all.at[rows_of(ypeers[1 - d], d * (rows // 2), rows // 2)]
        go(piece, piece, o_s.at[1, d], o_r.at[1, d], 'dm', ypeers[d])
    for d in range(2):
        got(o_all.at[rows_of(far, d * (rows // 2), rows // 2)], o_s.at[1, d], o_r.at[1, d], 'dm', ypeers[d])

    def tile_rows(owner, c, offset=0, count=share):
        return pl.ds(pl.multiple_of(c * (batch // 2) + owner * share + offset, xhalf), count)

    def tp_scatter(u):
        order = (xf, xn, xp, xi)
        for i, owner in enumerate(order):
            go(part.at[u, tile_rows(owner, 1 - core)], d2d_recv.at[u, i], d_s.at[u, i], d_r.at[u, i], 'tp', partner)
        for i, owner in enumerate(order):
            got(d2d_recv.at[u, i], d_s.at[u, i], d_r.at[u, i], 'tp', partner)
            here = tile_rows(owner, core)
            part[u, here] = part[u, here] + d2d_recv[u, i]
            if i == 0:
                for d in range(2):
                    go(part.at[u, tile_rows(xf, core, d * xhalf, xhalf)], xa_recv.at[u, d], xa_s.at[u, d], xa_r.at[u, d], 'tp', xpeer_ids[d])
            elif i < 3:
                d = i - 1
                go(part.at[u, tile_rows(owner, core, (1 - d) * xhalf, xhalf)], xb_recv.at[u, d], xb_s.at[u, d], xb_r.at[u, d], 'tp', xpeer_ids[d])
        for d in range(2):
            got(xa_recv.at[u, d], xa_s.at[u, d], xa_r.at[u, d], 'tp', xpeer_ids[d])
            xc_send[u, d] = xa_recv[u, d] + part[u, tile_rows(xpeers[d], core, d * xhalf, xhalf)]
            go(xc_send.at[u, d], xc_recv.at[u, d], xc_s.at[u, d], xc_r.at[u, d], 'tp', xpeer_ids[d])
        for d in range(2):
            got(xb_recv.at[u, d], xb_s.at[u, d], xb_r.at[u, d], 'tp', xpeer_ids[d])
            got(xc_recv.at[u, d], xc_s.at[u, d], xc_r.at[u, d], 'tp', xpeer_ids[d])
        return jnp.concatenate(
            [part[u, tile_rows(xi, core, d * xhalf, xhalf)] + xc_recv[u, d] + xb_recv[u, 1 - d] for d in range(2)], axis=0)

    def tp_gather(u, buf):
        mine = buf.at[tile_rows(xi, core)]
        for d in range(2):
            go(mine, mine, ag_s.at[u, d], ag_r.at[u, d], 'tp', xpeer_ids[d])
        go(mine, mine, agd_s.at[u, 0], agd_r.at[u, 0], 'tp', partner)
        for d in range(2):
            near = buf.at[tile_rows(xpeers[1 - d], core)]
            got(near, ag_s.at[u, d], ag_r.at[u, d], 'tp', xpeer_ids[d])
            piece = buf.at[tile_rows(xpeers[1 - d], core, d * xhalf, xhalf)]
            go(piece, piece, agf_s.at[u, d], agf_r.at[u, d], 'tp', xpeer_ids[d])
            go(near, near, agd_s.at[u, 1 + d], agd_r.at[u, 1 + d], 'tp', partner)
        for d in range(2):
            got(buf.at[tile_rows(xf, core, d * xhalf, xhalf)], agf_s.at[u, d], agf_r.at[u, d], 'tp', xpeer_ids[d])
        faraway = buf.at[tile_rows(xf, core)]
        go(faraway, faraway, agd_s.at[u, 3], agd_r.at[u, 3], 'tp', partner)
        for i, owner in enumerate((xi, xp, xn, xf)):
            got(buf.at[tile_rows(owner, 1 - core)], agd_s.at[u, i], agd_r.at[u, i], 'tp', partner)

    loads[0].wait()
    step = 256
    for n in range(0, width, step):
        part[0, :, n:n + step] = jnp.dot(o_all[...], wo[:, n:n + step], preferred_element_type=F32)
    attn = tp_scatter(0)
    h1 = (h_ref[tile_rows(xi, core)] + attn.astype(BF16))
    h1_buf[...] = h1
    h1 = h1.astype(F32)
    col = jnp.sum(h1 * h1, axis=-1, keepdims=True)
    ss_send[...] = column_to_row(jnp.concatenate([col] * (128 // share), axis=0))
    for i, peer in enumerate((nxt, prv, far)):
        go(ss_send, ss_recv.at[i], ss_s.at[i], ss_r.at[i], 'dm', peer)
    for i, peer in enumerate((nxt, prv, far)):
        got(ss_recv.at[i], ss_s.at[i], ss_r.at[i], 'dm', peer)
    total = ss_send[...] + ss_recv[0] + ss_recv[1] + ss_recv[2]
    scale = row_to_column(lax.rsqrt(total / width_full + EPS))[:share]
    x2_all[tile_rows(xi, core)] = scale_rows(h1, scale, g_ref[...].astype(F32))
    tp_gather(0, x2_all)

    loads[1].wait()
    loads[2].wait()

    def columns(owner):
        return pl.ds(pl.multiple_of(owner * own_cols, 16), own_cols)

    for i, owner in enumerate((far, nxt, prv, dm)):
        for j, w in enumerate((wg, wu)):
            y = lax.dot_general(w[columns(owner)], x2_all[...], (((1,), (1,)), ((), ())), preferred_element_type=F32)
            for p in range(PARTS):
                for s in range(2):
                    gu[i, p, s, j] = y[p * pc + s * ph:p * pc + (s + 1) * ph]
        for p in range(PARTS):
            if i == 0:
                for d in range(2):
                    go(gu.at[0, p, d], ga_recv.at[d, p], ga_s.at[d, p], ga_r.at[d, p], 'dm', ypeers[d])
            elif i < 3:
                d = i - 1
                go(gu.at[i, p, 1 - d], gb_recv.at[d, p], gb_s.at[d, p], gb_r.at[d, p], 'dm', ypeers[d])
    for p in range(PARTS):
        for d in range(2):
            got(ga_recv.at[d, p], ga_s.at[d, p], ga_r.at[d, p], 'dm', ypeers[d])
            gc_send[d, p] = ga_recv[d, p] + gu[1 + d, p, d]
            go(gc_send.at[d, p], gc_recv.at[d, p], gc_s.at[d, p], gc_r.at[d, p], 'dm', ypeers[d])

    cut = (pc // 2 + 15) // 16 * 16
    cuts = ((0, cut), (cut, pc - cut))

    def m_rows(owner, p, offset=0, count=pc):
        return pl.ds(pl.multiple_of(owner * own_cols + p * pc + offset, 16), count)

    for p in range(PARTS):
        halves = []
        for d in range(2):
            got(gb_recv.at[d, p], gb_s.at[d, p], gb_r.at[d, p], 'dm', ypeers[d])
            got(gc_recv.at[d, p], gc_s.at[d, p], gc_r.at[d, p], 'dm', ypeers[d])
        for d in range(2):
            gate, up = (gu[3, p, d, j] + gc_recv[d, p, j] + gb_recv[1 - d, p, j] for j in range(2))
            halves.append(gate * jax.nn.sigmoid(gate) * up)
        m_all[m_rows(dm, p)] = jnp.concatenate(halves, axis=0).astype(BF16)
        for d in range(2):
            mine = m_all.at[m_rows(dm, p)]
            go(mine, mine, m_s.at[d, p], m_r.at[d, p], 'dm', ypeers[d])
    for p in range(PARTS):
        for d in range(2):
            got(m_all.at[m_rows(ypeers[1 - d], p)], m_s.at[d, p], m_r.at[d, p], 'dm', ypeers[d])
            piece = m_all.at[m_rows(ypeers[1 - d], p, *cuts[d])]
            go(piece, piece, mf_s.at[d, p], mf_r.at[d, p], 'dm', ypeers[d])
    for p in range(PARTS):
        for d in range(2):
            got(m_all.at[m_rows(far, p, *cuts[d])], mf_s.at[d, p], mf_r.at[d, p], 'dm', ypeers[d])

    loads[3].wait()
    for n in range(0, width, step):
        part[1, :, n:n + step] = lax.dot_general(m_all[...], wd[:, n:n + step], (((0,), (0,)), ((), ())), preferred_element_type=F32)
    mlp = tp_scatter(1)
    h_all[tile_rows(xi, core)] = h1_buf[...] + mlp.astype(BF16)
    tp_gather(1, h_all)
    out_ref[...] = h_all[...]
    for copy in sends:
        copy.wait_send()


def mlp(nd, nx, o, hidden, g, wo, wg, wu, wd):
    batch, width = hidden.shape
    cols = wd.shape[0]
    inner = wo.shape[0]
    share = batch // (2 * nx)
    vmem = pl.BlockSpec(memory_space=pltpu.VMEM)
    hbm = pl.BlockSpec(memory_space=pl.ANY)
    dma = pltpu.SemaphoreType.DMA
    xpiece = pltpu.VMEM((2, 2, share // 2, width), F32)
    ph = cols // nd // PARTS // 2
    gpiece = pltpu.VMEM((2, PARTS, 2, ph, batch), F32)
    return pl.pallas_call(
        functools.partial(mlp_kernel, nd, nx, width * nd),
        out_shape=jax.ShapeDtypeStruct((batch, width), BF16),
        in_specs=[vmem] * 3 + [hbm] * 4,
        out_specs=vmem,
        scratch_shapes=[
            pltpu.VMEM(wo.shape, BF16), pltpu.VMEM(wg.shape, BF16), pltpu.VMEM(wu.shape, BF16), pltpu.VMEM(wd.shape, BF16),
            pltpu.VMEM((batch, inner), BF16), pltpu.VMEM((2, batch, width), F32), pltpu.VMEM((2, nx, share, width), F32),
            xpiece, xpiece, xpiece, xpiece, pltpu.VMEM((share, width), BF16), pltpu.VMEM((8, 128), F32), pltpu.VMEM((3, 8, 128), F32),
            pltpu.VMEM((batch, width), BF16), pltpu.VMEM((4, PARTS, 2, 2, ph, batch), F32), gpiece, gpiece, gpiece, gpiece,
            pltpu.VMEM((cols, batch), BF16), pltpu.VMEM((batch, width), BF16),
            dma((4,)), dma((2, 2)), dma((2, 2)), dma((2, 4)), dma((2, 4))] + [dma((2, 2))] * 6 + [dma((3,))] * 2
        + [dma((2, 2))] * 4 + [dma((2, 4))] * 2 + [dma((2, PARTS))] * 10,
        compiler_params=pltpu.CompilerParams(collective_id=1, has_side_effects=True, vmem_limit_bytes=56 * 2 ** 20),
        name='mlp',
    )(o, hidden, g, wo, wg, wu, wd)


def solution(mesh):
    nd, nx = mesh.shape['dm'], mesh.shape['tp'] // 2
    row_spec = P('dp', 'dm')
    cache_spec = P(('dp', 'dm'), None, 'tp', None)
    batch_spec = P(('dp', 'dm'))
    rope_spec = P(('dp', 'dm'), None)
    in_specs = (row_spec, P('dm', 'tp', None), P('dm', 'tp', None), P('dm', 'tp', None), P('tp', None, 'dm'), P('dm', 'tp'), P('dm', 'tp'), P('tp', 'dm'), P('dm'), P('dm'), cache_spec, cache_spec, batch_spec, rope_spec, rope_spec)
    out_specs = (row_spec, cache_spec, cache_spec)

    def local_layer(hidden, w_q, w_k, w_v, w_o, w_gate, w_up, w_down, norm_attn, norm_mlp, k_cache, v_cache, seq_lens, rope_cos, rope_sin):
        wq, wk, wv = (w.transpose(1, 0, 2) for w in (w_q, w_k, w_v))
        q, kn, vn = qkv(nd, hidden, norm_attn[None, :], rope_cos, rope_sin, wq, wk, wv)
        ko, vo, o = attend(seq_lens, q, kn, vn, k_cache.transpose(0, 2, 1, 3), v_cache.transpose(0, 2, 1, 3))
        h_out = mlp(nd, nx, o, hidden, norm_mlp[None, :], w_o.reshape(-1, w_o.shape[-1]), w_gate.T, w_up.T, w_down)
        return h_out, ko.transpose(0, 2, 1, 3), vo.transpose(0, 2, 1, 3)

    return jax.shard_map(local_layer, mesh=mesh, in_specs=in_specs, out_specs=out_specs, check_vma=False)
```

```python
import functools

import jax
import jax.numpy as jnp
from jax import lax
from jax.experimental import pallas as pl
from jax.experimental.pallas import tpu as pltpu
from jax.sharding import PartitionSpec as P

EPS = 1e-6
F32 = jnp.float32
BF16 = jnp.bfloat16
MESH = pl.DeviceIdType.MESH
VMEM_LIMIT = 63 * 2 ** 20
PARTS = 3


def remote(src, dst, send, recv, axis, index):
    return pltpu.make_async_remote_copy(
        src_ref=src, dst_ref=dst, send_sem=send, recv_sem=recv, device_id={axis: index}, device_id_type=MESH)


def entry_barrier(peers):
    barrier = pltpu.get_barrier_semaphore()
    for axis, index in peers:
        pl.semaphore_signal(barrier, inc=1, device_id={axis: index}, device_id_type=MESH)
    return lambda: pl.semaphore_wait(barrier, len(peers))


def column_to_row(col):
    rows = col.shape[0]
    return jnp.concatenate(
        [jnp.broadcast_to(col[i:i + 128], (128, 128)).T[:8] for i in range(0, rows, 128)], axis=1)


def row_to_column(row):
    rows = row.shape[1]
    return jnp.concatenate(
        [jnp.broadcast_to(row[:1, i:i + 128], (128, 128)).T for i in range(0, rows, 128)], axis=0)


def scale_rows(x, scale, gain):
    width = x.shape[1]
    cols = [x[:, i:i + 128] * scale * gain[:, i:i + 128] for i in range(0, width, 128)]
    return jnp.concatenate(cols, axis=1).astype(BF16)


def qkv_kernel(nd, width_full, h_hbm, g_hbm, cos_hbm, sin_hbm, wq_hbm, wk_hbm, wv_hbm, q_out, k_out, v_out,
               h_ref, g_ref, cos_ref, sin_ref, w_buf, x_buf, part, ss_send, ss_recv, a_recv, b_recv, c_send, c_recv, cos2, sin2,
               in_sem, w_sem, ss_s, ss_r, a_s, a_r, b_s, b_r, c_s, c_r):
    dm = lax.axis_index('dm')
    nxt, prv, far = lax.rem(dm + 1, nd), lax.rem(dm + nd - 1, nd), lax.rem(dm + 2, nd)
    rows = h_ref.shape[0] // nd
    half = rows // 2
    heads = w_buf.shape[1]

    wait_barrier = entry_barrier([('dm', nxt), ('dm', prv), ('dm', far)])
    small = [pltpu.make_async_copy(src, dst, in_sem.at[i]) for i, (src, dst) in enumerate(
        ((h_hbm, h_ref), (g_hbm, g_ref), (cos_hbm, cos_ref), (sin_hbm, sin_ref)))]
    loads = [pltpu.make_async_copy(src, w_buf.at[t], w_sem.at[t]) for t, src in enumerate((wq_hbm, wk_hbm, wv_hbm))]
    for load in small + loads:
        load.start()

    small[0].wait()
    x = h_ref[...].astype(F32)
    ss_send[...] = column_to_row(jnp.sum(x * x, axis=-1, keepdims=True))
    wait_barrier()
    ss = [remote(ss_send, ss_recv.at[i], ss_s.at[i], ss_r.at[i], 'dm', peer) for i, peer in enumerate((nxt, prv, far))]
    for copy in ss:
        copy.start()
    for load in small[1:]:
        load.wait()
    hd = cos_ref.shape[1]
    cos2[:, :hd] = cos_ref[...]
    cos2[:, hd:] = cos_ref[...]
    sin2[:, :hd] = -sin_ref[...]
    sin2[:, hd:] = sin_ref[...]
    for copy in ss:
        copy.wait_recv()
    total = ss_send[...] + ss_recv[0] + ss_recv[1] + ss_recv[2]
    scale = row_to_column(lax.rsqrt(total / width_full + EPS))
    x_buf[...] = scale_rows(h_ref[...].astype(F32), scale, g_ref[...].astype(F32)[None, :])

    def block(owner, second):
        return pl.ds(pl.multiple_of(owner * rows + second * half, half), half)

    peers = (nxt, prv)
    sends = []
    for t in range(3):
        loads[t].wait()
        for hh in range(heads):
            part[t, :, hh * 128:(hh + 1) * 128] = jnp.dot(x_buf[...], w_buf[t, hh], preferred_element_type=F32)
        for d in range(2):
            sends.append(remote(part.at[t, block(far, d)], a_recv.at[d, t], a_s.at[d, t], a_r.at[d, t], 'dm', peers[d]))
            sends[-1].start()
        for d in range(2):
            sends.append(remote(part.at[t, block(peers[d], 1 - d)], b_recv.at[d, t], b_s.at[d, t], b_r.at[d, t], 'dm', peers[d]))
            sends[-1].start()
    for t in range(3):
        for d in range(2):
            remote(a_recv.at[d, t], a_recv.at[d, t], a_s.at[d, t], a_r.at[d, t], 'dm', peers[d]).wait_recv()
            c_send[d, t] = a_recv[d, t] + part[t, block(peers[d], d)]
            sends.append(remote(c_send.at[d, t], c_recv.at[d, t], c_s.at[d, t], c_r.at[d, t], 'dm', peers[d]))
            sends[-1].start()
    for t, out in enumerate((q_out, k_out, v_out)):
        for d in range(2):
            remote(b_recv.at[d, t], b_recv.at[d, t], b_s.at[d, t], b_r.at[d, t], 'dm', peers[d]).wait_recv()
            remote(c_recv.at[d, t], c_recv.at[d, t], c_s.at[d, t], c_r.at[d, t], 'dm', peers[d]).wait_recv()
        for d in range(2):
            tot = part[t, block(dm, d)] + c_recv[d, t] + b_recv[1 - d, t]
            for hh in range(heads):
                y = tot[:, hh * 128:(hh + 1) * 128]
                if t < 2:
                    here = slice(d * half, (d + 1) * half)
                    y = y * cos2[here] + pltpu.roll(y, 64, 1) * sin2[here]
                out[d * half:(d + 1) * half, hh * 128:(hh + 1) * 128] = y.astype(BF16).astype(F32)
    for copy in ss + sends:
        copy.wait_send()


def qkv(nd, hidden, g, cos, sin, wq, wk, wv):
    batch, width = hidden.shape
    heads, _, head = wq.shape
    rows, cols = batch // nd, heads * head
    half = rows // 2
    vmem = pl.BlockSpec(memory_space=pltpu.VMEM)
    hbm = pl.BlockSpec(memory_space=pl.ANY)
    dma = pltpu.SemaphoreType.DMA
    piece = pltpu.VMEM((2, 3, half, cols), F32)
    return pl.pallas_call(
        functools.partial(qkv_kernel, nd, width * nd),
        out_shape=[jax.ShapeDtypeStruct((rows, cols), F32)] * 3,
        in_specs=[hbm] * 7,
        out_specs=[vmem] * 3,
        scratch_shapes=[
            pltpu.VMEM(hidden.shape, BF16), pltpu.VMEM(g.shape, BF16), pltpu.VMEM(cos.shape, F32), pltpu.VMEM(sin.shape, F32),
            pltpu.VMEM((3, heads, width, head), BF16), pltpu.VMEM((batch, width), BF16), pltpu.VMEM((3, batch, cols), F32),
            pltpu.VMEM((8, batch), F32), pltpu.VMEM((3, 8, batch), F32), piece, piece, piece, piece,
            pltpu.VMEM((rows, head), F32), pltpu.VMEM((rows, head), F32),
            dma((4,)), dma((3,)), dma((3,)), dma((3,))] + [dma((2, 3))] * 6,
        compiler_params=pltpu.CompilerParams(collective_id=0, has_side_effects=True, vmem_limit_bytes=VMEM_LIMIT),
        name='qkv',
    )(hidden, g, cos, sin, wq, wk, wv)


def attend_kernel(lens_ref, q_ref, kn_ref, vn_ref, kc_ref, vc_ref, ko_ref, vo_ref, o_ref):
    step = pl.program_id(0)
    rb, heads, slots, head = kc_ref.shape
    window = 16
    span = heads * slots
    pos = lax.broadcasted_iota(jnp.int32, (heads, window, head), 1)
    head_row = lax.broadcasted_iota(jnp.int32, (8, span), 0)
    lane = lax.broadcasted_iota(jnp.int32, (8, span), 1)
    lane_slot = lane % slots
    own_head = (lane // slots) == head_row
    q_row = lax.broadcasted_iota(jnp.int32, (8, head), 0)
    q_all = q_ref[...]
    ko_ref[...] = kc_ref[...]
    vo_ref[...] = vc_ref[...]
    lengths = [lens_ref[step * rb + r] for r in range(rb)]
    for r in range(rb):
        base = pl.multiple_of(lengths[r] // window * window, window)
        write = pos == lengths[r] - base
        for new_ref, old, out in ((kn_ref, kc_ref, ko_ref), (vn_ref, vc_ref, vo_ref)):
            new = jnp.stack([jnp.broadcast_to(new_ref[r:r + 1, i * head:(i + 1) * head], (window, head)) for i in range(heads)])
            out[r, :, pl.ds(base, window), :] = jnp.where(write, new, old[r, :, pl.ds(base, window), :].astype(F32)).astype(BF16)
    scores, masks = [], []
    for r in range(rb):
        q = jnp.zeros((8, head), F32)
        for i in range(heads):
            q = jnp.where(q_row == i, jnp.broadcast_to(q_all[r:r + 1, i * head:(i + 1) * head], (8, head)), q)
        k = ko_ref[r].reshape(span, head)
        s = lax.dot_general(q.astype(BF16), k, (((1,), (1,)), ((), ())), preferred_element_type=F32)
        masks.append(own_head & (lane_slot <= lengths[r]))
        scores.append(jnp.where(masks[r], s * (head ** -0.5), float(jnp.finfo(F32).min)))
    s = jnp.stack(scores)
    p = jnp.exp(s - jnp.max(s, axis=-1, keepdims=True))
    p = jnp.where(jnp.stack(masks), p, 0.0)
    p = (p / jnp.maximum(jnp.sum(p, axis=-1, keepdims=True), 1e-30)).astype(BF16)
    for r in range(rb):
        o = jnp.dot(p[r], vo_ref[r].reshape(span, head), preferred_element_type=F32)
        for i in range(heads):
            o_ref[r:r + 1, i * head:(i + 1) * head] = o[i:i + 1]


def attend(lens, q, kn, vn, kc, vc):
    rows, heads, slots, head = kc.shape
    rb = 8
    row_block = pl.BlockSpec((rb, heads * head), lambda i, lens: (i, 0))
    cache_block = pl.BlockSpec((rb, heads, slots, head), lambda i, lens: (i, 0, 0, 0))
    return pl.pallas_call(
        attend_kernel,
        grid_spec=pltpu.PrefetchScalarGridSpec(
            num_scalar_prefetch=1, grid=(rows // rb,),
            in_specs=[row_block] * 3 + [cache_block] * 2,
            out_specs=[cache_block, cache_block, row_block]),
        out_shape=[jax.ShapeDtypeStruct(kc.shape, BF16), jax.ShapeDtypeStruct(vc.shape, BF16),
                   jax.ShapeDtypeStruct((rows, heads * head), F32)],
        compiler_params=pltpu.CompilerParams(vmem_limit_bytes=VMEM_LIMIT),
        cost_estimate=pl.CostEstimate(flops=4 * rows * heads * slots * head, bytes_accessed=4 * kc.size * 2, transcendentals=0),
        name='attend',
    )(lens, q, kn, vn, kc, vc)


def mlp_kernel(nd, nx, width_full, o_ref, h_hbm, g_hbm, wo_hbm, wg_hbm, wu_hbm, wd_hbm, out_ref,
               h_ref, g_ref, wo, wg, wu, wd, o_all, part, d2d_recv, xa_recv, xb_recv, xc_send, xc_recv, h1_buf, ss_send, ss_recv,
               x2_all, gu, ga_recv, gb_recv, gc_send, gc_recv, m_all, h_all,
               w_sem, o_s, o_r, d_s, d_r, xa_s, xa_r, xb_s, xb_r, xc_s, xc_r, ss_s, ss_r,
               ag_s, ag_r, agf_s, agf_r, agd_s, agd_r, ga_s, ga_r, gb_s, gb_r, gc_s, gc_r, m_s, m_r, mf_s, mf_r):
    dm, tp = lax.axis_index('dm'), lax.axis_index('tp')
    nxt, prv, far = lax.rem(dm + 1, nd), lax.rem(dm + nd - 1, nd), lax.rem(dm + 2, nd)
    core, xi = lax.rem(tp, 2), tp // 2
    xn, xp, xf = lax.rem(xi + 1, nx), lax.rem(xi + nx - 1, nx), lax.rem(xi + 2, nx)
    partner = tp + 1 - 2 * core
    ypeers, xpeers, xpeer_ids = (nxt, prv), (xn, xp), (2 * xn + core, 2 * xp + core)
    batch, width = h_ref.shape
    rows = batch // nd
    share = batch // (2 * nx)
    xhalf = share // 2
    cols = wd.shape[0]
    own_cols = cols // nd
    pc = own_cols // PARTS
    ph = pc // 2
    sends = []

    def go(*args):
        sends.append(remote(*args))
        sends[-1].start()

    def got(ref, send, recv, axis, index):
        remote(ref, ref, send, recv, axis, index).wait_recv()

    wait_barrier = entry_barrier([('dm', nxt), ('dm', prv), ('dm', far), ('tp', partner), ('tp', xpeer_ids[0]), ('tp', xpeer_ids[1])])
    loads = [pltpu.make_async_copy(src, dst, w_sem.at[i])
             for i, (src, dst) in enumerate(((wo_hbm, wo), (wg_hbm, wg), (wu_hbm, wu), (wd_hbm, wd), (h_hbm, h_ref), (g_hbm, g_ref)))]
    for load in loads:
        load.start()

    def rows_of(owner, offset=0, count=rows):
        return pl.ds(pl.multiple_of(owner * rows + offset, 16), count)

    o_all[rows_of(dm)] = o_ref[...].astype(BF16)
    wait_barrier()
    for d in range(2):
        mine = o_all.at[rows_of(dm)]
        go(mine, mine, o_s.at[0, d], o_r.at[0, d], 'dm', ypeers[d])
    for d in range(2):
        near = o_all.at[rows_of(ypeers[1 - d])]
        got(near, o_s.at[0, d], o_r.at[0, d], 'dm', ypeers[d])
        piece = o_all.at[rows_of(ypeers[1 - d], d * (rows // 2), rows // 2)]
        go(piece, piece, o_s.at[1, d], o_r.at[1, d], 'dm', ypeers[d])
    for d in range(2):
        got(o_all.at[rows_of(far, d * (rows // 2), rows // 2)], o_s.at[1, d], o_r.at[1, d], 'dm', ypeers[d])

    def tile_rows(owner, c, offset=0, count=share):
        return pl.ds(pl.multiple_of(c * (batch // 2) + owner * share + offset, xhalf), count)

    def tp_scatter(u):
        order = (xf, xn, xp, xi)
        for i, owner in enumerate(order):
            go(part.at[u, tile_rows(owner, 1 - core)], d2d_recv.at[u, i], d_s.at[u, i], d_r.at[u, i], 'tp', partner)
        for i, owner in enumerate(order):
            got(d2d_recv.at[u, i], d_s.at[u, i], d_r.at[u, i], 'tp', partner)
            here = tile_rows(owner, core)
            part[u, here] = part[u, here] + d2d_recv[u, i]
            if i == 0:
                for d in range(2):
                    go(part.at[u, tile_rows(xf, core, d * xhalf, xhalf)], xa_recv.at[u, d], xa_s.at[u, d], xa_r.at[u, d], 'tp', xpeer_ids[d])
            elif i < 3:
                d = i - 1
                go(part.at[u, tile_rows(owner, core, (1 - d) * xhalf, xhalf)], xb_recv.at[u, d], xb_s.at[u, d], xb_r.at[u, d], 'tp', xpeer_ids[d])
        for d in range(2):
            got(xa_recv.at[u, d], xa_s.at[u, d], xa_r.at[u, d], 'tp', xpeer_ids[d])
            xc_send[u, d] = xa_recv[u, d] + part[u, tile_rows(xpeers[d], core, d * xhalf, xhalf)]
            go(xc_send.at[u, d], xc_recv.at[u, d], xc_s.at[u, d], xc_r.at[u, d], 'tp', xpeer_ids[d])
        for d in range(2):
            got(xb_recv.at[u, d], xb_s.at[u, d], xb_r.at[u, d], 'tp', xpeer_ids[d])
            got(xc_recv.at[u, d], xc_s.at[u, d], xc_r.at[u, d], 'tp', xpeer_ids[d])
        return jnp.concatenate(
            [part[u, tile_rows(xi, core, d * xhalf, xhalf)] + xc_recv[u, d] + xb_recv[u, 1 - d] for d in range(2)], axis=0)

    def tp_gather(u, buf):
        mine = buf.at[tile_rows(xi, core)]
        for d in range(2):
            go(mine, mine, ag_s.at[u, d], ag_r.at[u, d], 'tp', xpeer_ids[d])
        go(mine, mine, agd_s.at[u, 0], agd_r.at[u, 0], 'tp', partner)
        for d in range(2):
            near = buf.at[tile_rows(xpeers[1 - d], core)]
            got(near, ag_s.at[u, d], ag_r.at[u, d], 'tp', xpeer_ids[d])
            piece = buf.at[tile_rows(xpeers[1 - d], core, d * xhalf, xhalf)]
            go(piece, piece, agf_s.at[u, d], agf_r.at[u, d], 'tp', xpeer_ids[d])
            go(near, near, agd_s.at[u, 1 + d], agd_r.at[u, 1 + d], 'tp', partner)
        for d in range(2):
            got(buf.at[tile_rows(xf, core, d * xhalf, xhalf)], agf_s.at[u, d], agf_r.at[u, d], 'tp', xpeer_ids[d])
        faraway = buf.at[tile_rows(xf, core)]
        go(faraway, faraway, agd_s.at[u, 3], agd_r.at[u, 3], 'tp', partner)
        for i, owner in enumerate((xi, xp, xn, xf)):
            got(buf.at[tile_rows(owner, 1 - core)], agd_s.at[u, i], agd_r.at[u, i], 'tp', partner)

    loads[0].wait()
    step = 256
    for n in range(0, width, step):
        part[0, :, n:n + step] = jnp.dot(o_all[...], wo[:, n:n + step], preferred_element_type=F32)
    attn = tp_scatter(0)
    loads[4].wait()
    loads[5].wait()
    h1 = (h_ref[tile_rows(xi, core)] + attn.astype(BF16))
    h1_buf[...] = h1
    h1 = h1.astype(F32)
    col = jnp.sum(h1 * h1, axis=-1, keepdims=True)
    ss_send[...] = column_to_row(jnp.concatenate([col] * (128 // share), axis=0))
    for i, peer in enumerate((nxt, prv, far)):
        go(ss_send, ss_recv.at[i], ss_s.at[i], ss_r.at[i], 'dm', peer)
    for i, peer in enumerate((nxt, prv, far)):
        got(ss_recv.at[i], ss_s.at[i], ss_r.at[i], 'dm', peer)
    total = ss_send[...] + ss_recv[0] + ss_recv[1] + ss_recv[2]
    scale = row_to_column(lax.rsqrt(total / width_full + EPS))[:share]
    x2_all[tile_rows(xi, core)] = scale_rows(h1, scale, g_ref[...].astype(F32)[None, :])
    tp_gather(0, x2_all)

    loads[1].wait()
    loads[2].wait()

    def columns(owner):
        return pl.ds(pl.multiple_of(owner * own_cols, 16), own_cols)

    for i, owner in enumerate((far, nxt, prv, dm)):
        for j, w in enumerate((wg, wu)):
            y = lax.dot_general(w[columns(owner)], x2_all[...], (((1,), (1,)), ((), ())), preferred_element_type=F32)
            for p in range(PARTS):
                for s in range(2):
                    gu[i, p, s, j] = y[p * pc + s * ph:p * pc + (s + 1) * ph]
        for p in range(PARTS):
            if i == 0:
                for d in range(2):
                    go(gu.at[0, p, d], ga_recv.at[d, p], ga_s.at[d, p], ga_r.at[d, p], 'dm', ypeers[d])
            elif i < 3:
                d = i - 1
                go(gu.at[i, p, 1 - d], gb_recv.at[d, p], gb_s.at[d, p], gb_r.at[d, p], 'dm', ypeers[d])
    for p in range(PARTS):
        for d in range(2):
            got(ga_recv.at[d, p], ga_s.at[d, p], ga_r.at[d, p], 'dm', ypeers[d])
            gc_send[d, p] = ga_recv[d, p] + gu[1 + d, p, d]
            go(gc_send.at[d, p], gc_recv.at[d, p], gc_s.at[d, p], gc_r.at[d, p], 'dm', ypeers[d])

    cut = (pc // 2 + 15) // 16 * 16
    cuts = ((0, cut), (cut, pc - cut))

    def m_rows(owner, p, offset=0, count=pc):
        return pl.ds(pl.multiple_of(owner * own_cols + p * pc + offset, 16), count)

    for p in range(PARTS):
        halves = []
        for d in range(2):
            got(gb_recv.at[d, p], gb_s.at[d, p], gb_r.at[d, p], 'dm', ypeers[d])
            got(gc_recv.at[d, p], gc_s.at[d, p], gc_r.at[d, p], 'dm', ypeers[d])
        for d in range(2):
            gate, up = (gu[3, p, d, j] + gc_recv[d, p, j] + gb_recv[1 - d, p, j] for j in range(2))
            halves.append(gate * jax.nn.sigmoid(gate) * up)
        m_all[m_rows(dm, p)] = jnp.concatenate(halves, axis=0).astype(BF16)
        for d in range(2):
            mine = m_all.at[m_rows(dm, p)]
            go(mine, mine, m_s.at[d, p], m_r.at[d, p], 'dm', ypeers[d])
    for p in range(PARTS):
        for d in range(2):
            got(m_all.at[m_rows(ypeers[1 - d], p)], m_s.at[d, p], m_r.at[d, p], 'dm', ypeers[d])
            piece = m_all.at[m_rows(ypeers[1 - d], p, *cuts[d])]
            go(piece, piece, mf_s.at[d, p], mf_r.at[d, p], 'dm', ypeers[d])
    for p in range(PARTS):
        for d in range(2):
            got(m_all.at[m_rows(far, p, *cuts[d])], mf_s.at[d, p], mf_r.at[d, p], 'dm', ypeers[d])

    loads[3].wait()
    for n in range(0, width, step):
        part[1, :, n:n + step] = lax.dot_general(m_all[...], wd[:, n:n + step], (((0,), (0,)), ((), ())), preferred_element_type=F32)
    mlp = tp_scatter(1)
    h_all[tile_rows(xi, core)] = h1_buf[...] + mlp.astype(BF16)
    tp_gather(1, h_all)
    out_ref[...] = h_all[...]
    for copy in sends:
        copy.wait_send()


def mlp(nd, nx, o, hidden, g, wo, wg, wu, wd):
    batch, width = hidden.shape
    cols = wd.shape[0]
    inner = wo.shape[0]
    share = batch // (2 * nx)
    vmem = pl.BlockSpec(memory_space=pltpu.VMEM)
    hbm = pl.BlockSpec(memory_space=pl.ANY)
    dma = pltpu.SemaphoreType.DMA
    xpiece = pltpu.VMEM((2, 2, share // 2, width), F32)
    ph = cols // nd // PARTS // 2
    gpiece = pltpu.VMEM((2, PARTS, 2, ph, batch), F32)
    return pl.pallas_call(
        functools.partial(mlp_kernel, nd, nx, width * nd),
        out_shape=jax.ShapeDtypeStruct((batch, width), BF16),
        in_specs=[vmem] + [hbm] * 6,
        out_specs=vmem,
        scratch_shapes=[
            pltpu.VMEM(hidden.shape, BF16), pltpu.VMEM(g.shape, BF16),
            pltpu.VMEM(wo.shape, BF16), pltpu.VMEM(wg.shape, BF16), pltpu.VMEM(wu.shape, BF16), pltpu.VMEM(wd.shape, BF16),
            pltpu.VMEM((batch, inner), BF16), pltpu.VMEM((2, batch, width), F32), pltpu.VMEM((2, nx, share, width), F32),
            xpiece, xpiece, xpiece, xpiece, pltpu.VMEM((share, width), BF16), pltpu.VMEM((8, 128), F32), pltpu.VMEM((3, 8, 128), F32),
            pltpu.VMEM((batch, width), BF16), pltpu.VMEM((4, PARTS, 2, 2, ph, batch), F32), gpiece, gpiece, gpiece, gpiece,
            pltpu.VMEM((cols, batch), BF16), pltpu.VMEM((batch, width), BF16),
            dma((6,)), dma((2, 2)), dma((2, 2)), dma((2, 4)), dma((2, 4))] + [dma((2, 2))] * 6 + [dma((3,))] * 2
        + [dma((2, 2))] * 4 + [dma((2, 4))] * 2 + [dma((2, PARTS))] * 10,
        compiler_params=pltpu.CompilerParams(collective_id=1, has_side_effects=True, vmem_limit_bytes=VMEM_LIMIT),
        name='mlp',
    )(o, hidden, g, wo, wg, wu, wd)


def solution(mesh):
    nd, nx = mesh.shape['dm'], mesh.shape['tp'] // 2
    row_spec = P('dp', 'dm')
    cache_spec = P(('dp', 'dm'), None, 'tp', None)
    batch_spec = P(('dp', 'dm'))
    rope_spec = P(('dp', 'dm'), None)
    in_specs = (row_spec, P('dm', 'tp', None), P('dm', 'tp', None), P('dm', 'tp', None), P('tp', None, 'dm'), P('dm', 'tp'), P('dm', 'tp'), P('tp', 'dm'), P('dm'), P('dm'), cache_spec, cache_spec, batch_spec, rope_spec, rope_spec)
    out_specs = (row_spec, cache_spec, cache_spec)

    def local_layer(hidden, w_q, w_k, w_v, w_o, w_gate, w_up, w_down, norm_attn, norm_mlp, k_cache, v_cache, seq_lens, rope_cos, rope_sin):
        wq, wk, wv = (w.transpose(1, 0, 2) for w in (w_q, w_k, w_v))
        q, kn, vn = qkv(nd, hidden, norm_attn, rope_cos, rope_sin, wq, wk, wv)
        ko, vo, o = attend(seq_lens, q, kn, vn, k_cache.transpose(0, 2, 1, 3), v_cache.transpose(0, 2, 1, 3))
        h_out = mlp(nd, nx, o, hidden, norm_mlp, w_o.reshape(-1, w_o.shape[-1]), w_gate.T, w_up.T, w_down)
        return h_out, ko.transpose(0, 2, 1, 3), vo.transpose(0, 2, 1, 3)

    return jax.shard_map(local_layer, mesh=mesh, in_specs=in_specs, out_specs=out_specs, check_vma=False)
```

```python
import functools

import jax
import jax.numpy as jnp
from jax import lax
from jax.experimental import pallas as pl
from jax.experimental.pallas import tpu as pltpu
from jax.sharding import PartitionSpec as P

EPS = 1e-6
F32 = jnp.float32
BF16 = jnp.bfloat16
MESH = pl.DeviceIdType.MESH
VMEM_LIMIT = 63 * 2 ** 20
BATCHES = 2
PARTS = 3


def remote(src, dst, send, recv, axis, index):
    return pltpu.make_async_remote_copy(
        src_ref=src, dst_ref=dst, send_sem=send, recv_sem=recv, device_id={axis: index}, device_id_type=MESH)


def entry_barrier(peers):
    barrier = pltpu.get_barrier_semaphore()
    for axis, index in peers:
        pl.semaphore_signal(barrier, inc=1, device_id={axis: index}, device_id_type=MESH)
    return lambda: pl.semaphore_wait(barrier, len(peers))


def column_to_row(col):
    rows = col.shape[0]
    return jnp.concatenate(
        [jnp.broadcast_to(col[i:i + 128], (128, 128)).T[:8] for i in range(0, rows, 128)], axis=1)


def row_to_column(row):
    rows = row.shape[1]
    return jnp.concatenate(
        [jnp.broadcast_to(row[:1, i:i + 128], (128, 128)).T for i in range(0, rows, 128)], axis=0)


def scale_rows(x, scale, gain):
    width = x.shape[1]
    cols = [x[:, i:i + 128] * scale * gain[:, i:i + 128] for i in range(0, width, 128)]
    return jnp.concatenate(cols, axis=1).astype(BF16)


def layer_kernel(nd, nx, width_full, lens_ref, h_hbm, g1_hbm, g2_hbm, cos_hbm, sin_hbm, wq_hbm, wk_hbm, wv_hbm, wo_hbm, wg_hbm, wu_hbm, wd_hbm,
                 kc_hbm, vc_hbm, out_ref, k_out, v_out,
                 h_ref, g1_ref, g2_ref, cos_ref, sin_ref, wqkv, wo, wg, wu, wd, kc, vc,
                 x_buf, part, ss_send, ss_recv, a_recv, b_recv, c_send, c_recv, cos2, sin2, q_buf, o_own,
                 o_all, full, d2d_recv, xa_recv, xb_recv, xc_send, xc_recv, h1_buf, st_send, st_recv, x2_all,
                 gu, ga_recv, gb_recv, gc_send, gc_recv, m_all, h_all,
                 w_sem, ss_s, ss_r, a_s, a_r, b_s, b_r, c_s, c_r, o_s, o_r, d_s, d_r, xa_s, xa_r, xb_s, xb_r, xc_s, xc_r,
                 st_s, st_r, ag_s, ag_r, agf_s, agf_r, agd_s, agd_r, ga_s, ga_r, gb_s, gb_r, gc_s, gc_r, m_s, m_r, mf_s, mf_r):
    dm, tp = lax.axis_index('dm'), lax.axis_index('tp')
    nxt, prv, far = lax.rem(dm + 1, nd), lax.rem(dm + nd - 1, nd), lax.rem(dm + 2, nd)
    core, xi = lax.rem(tp, 2), tp // 2
    xn, xp, xf = lax.rem(xi + 1, nx), lax.rem(xi + nx - 1, nx), lax.rem(xi + 2, nx)
    partner = tp + 1 - 2 * core
    ypeers, xpeers, xids = (nxt, prv), (xn, xp), (2 * xn + core, 2 * xp + core)
    batch, width = h_ref.shape
    heads, slots, head = kc.shape[1:]
    rows = batch // nd
    rb = rows // BATCHES
    rh = rb // 2
    brows = nd * rb
    share = brows // (2 * nx)
    sh = share // 2
    cols = wd.shape[0]
    own_cols = cols // nd
    pc = own_cols // PARTS
    ph = pc // 2
    sends = []

    def go(*args):
        sends.append(remote(*args))
        sends[-1].start()

    def got(ref, send, recv, axis, index):
        remote(ref, ref, send, recv, axis, index).wait_recv()

    def al(x, n):
        return pl.multiple_of(x, n)

    wait_barrier = entry_barrier([('dm', nxt), ('dm', prv), ('dm', far), ('tp', partner), ('tp', xids[0]), ('tp', xids[1])])
    pairs = ((h_hbm, h_ref), (wq_hbm, wqkv.at[0]), (wk_hbm, wqkv.at[1]), (wv_hbm, wqkv.at[2]), (g1_hbm, g1_ref), (cos_hbm, cos_ref), (sin_hbm, sin_ref),
             (kc_hbm, kc), (vc_hbm, vc), (wo_hbm, wo), (g2_hbm, g2_ref), (wg_hbm, wg), (wu_hbm, wu), (wd_hbm, wd))
    loads = [pltpu.make_async_copy(src, dst, w_sem.at[i]) for i, (src, dst) in enumerate(pairs)]
    for load in loads[:7]:
        load.start()
    loads[0].wait()
    x = h_ref[...].astype(F32)
    ss_send[...] = column_to_row(jnp.sum(x * x, axis=-1, keepdims=True))
    wait_barrier()
    for i, peer in enumerate((nxt, prv, far)):
        go(ss_send, ss_recv.at[i], ss_s.at[i], ss_r.at[i], 'dm', peer)
    for load in loads[4:7]:
        load.wait()
    hd = cos_ref.shape[1]
    cos2[:, :hd] = cos_ref[...]
    cos2[:, hd:] = cos_ref[...]
    sin2[:, :hd] = -sin_ref[...]
    sin2[:, hd:] = sin_ref[...]
    for i, peer in enumerate((nxt, prv, far)):
        got(ss_recv.at[i], ss_s.at[i], ss_r.at[i], 'dm', peer)
    for load in loads[1:4]:
        load.wait()
    for load in loads[7:]:
        load.start()
    total = ss_send[...] + ss_recv[0] + ss_recv[1] + ss_recv[2]
    scale = row_to_column(lax.rsqrt(total / width_full + EPS))
    x_buf[...] = scale_rows(h_ref[...].astype(F32), scale, g1_ref[...].astype(F32)[None, :])

    def prow(owner, b, s):
        return pl.ds(al(owner * rows + b * rb + s * rh, rh), rh)

    def qkv_a(b, t):
        for d in range(2):
            go(part.at[t, prow(far, b, d)], a_recv.at[b, d, t], a_s.at[b, d, t], a_r.at[b, d, t], 'dm', ypeers[d])

    def qkv_b(b, t):
        for d in range(2):
            go(part.at[t, prow(ypeers[d], b, 1 - d)], b_recv.at[b, d, t], b_s.at[b, d, t], b_r.at[b, d, t], 'dm', ypeers[d])

    def qkv_c(b, t):
        for d in range(2):
            got(a_recv.at[b, d, t], a_s.at[b, d, t], a_r.at[b, d, t], 'dm', ypeers[d])
            c_send[b, d, t] = a_recv[b, d, t] + part[t, prow(ypeers[d], b, d)]
            go(c_send.at[b, d, t], c_recv.at[b, d, t], c_s.at[b, d, t], c_r.at[b, d, t], 'dm', ypeers[d])

    def totals(b):
        for t, out in enumerate((q_buf, k_out, v_out)):
            for d in range(2):
                got(b_recv.at[b, d, t], b_s.at[b, d, t], b_r.at[b, d, t], 'dm', ypeers[d])
                got(c_recv.at[b, d, t], c_s.at[b, d, t], c_r.at[b, d, t], 'dm', ypeers[d])
            for d in range(2):
                tot = part[t, prow(dm, b, d)] + c_recv[b, d, t] + b_recv[b, 1 - d, t]
                here = slice(b * rb + d * rh, b * rb + (d + 1) * rh)
                for i in range(heads):
                    y = tot[:, i * head:(i + 1) * head]
                    if t < 2:
                        y = y * cos2[here] + pltpu.roll(y, head // 2, 1) * sin2[here]
                    out[here, i * head:(i + 1) * head] = y.astype(BF16).astype(F32)

    span = heads * slots
    group = 8

    def attention(lo, hi):
        lane = lax.broadcasted_iota(jnp.int32, (8, span), 1)
        lane_slot = lane % slots
        own_head = (lane // slots) == lax.broadcasted_iota(jnp.int32, (8, span), 0)
        head_row = lax.broadcasted_iota(jnp.int32, (8, head), 0)

        def body(g, carry):
            first = al(g * group, group)
            vals = [ref[pl.ds(first, group), :] for ref in (q_buf, k_out, v_out)]

            def per_head(val, r):
                y = jnp.zeros((8, head), F32)
                for i in range(heads):
                    y = jnp.where(head_row == i, jnp.broadcast_to(val[r:r + 1, i * head:(i + 1) * head], (8, head)), y)
                return y

            scores, masks, news = [], [], []
            for r in range(group):
                q = per_head(vals[0], r)
                k = kc[first + r].reshape(span, head)
                s = lax.dot_general(q.astype(BF16), k, (((1,), (1,)), ((), ())), preferred_element_type=F32)
                masks.append(own_head & (lane_slot < lens_ref[first + r]))
                scores.append(jnp.where(masks[r], s * (head ** -0.5), float(jnp.finfo(F32).min)))
                news.append(jnp.sum(q * per_head(vals[1], r), axis=-1, keepdims=True) * (head ** -0.5))
            s, new = jnp.stack(scores), jnp.stack(news)
            top = jnp.maximum(jnp.max(s, axis=-1, keepdims=True), new)
            p = jnp.where(jnp.stack(masks), jnp.exp(s - top), 0.0)
            p_new = jnp.exp(new - top)
            den = jnp.sum(p, axis=-1, keepdims=True) + p_new
            p = (p / den).astype(BF16)
            p_new = (p_new / den).astype(BF16).astype(F32)
            for r in range(group):
                o = jnp.dot(p[r], vc[first + r].reshape(span, head), preferred_element_type=F32) + p_new[r] * per_head(vals[2], r)
                for i in range(heads):
                    o_own[g, r:r + 1, i * head:(i + 1) * head] = o[i:i + 1]
            return carry

        lax.fori_loop(lo, hi, body, 0)

    def orow(owner, s=0, n=rb):
        return pl.ds(al(owner * rb + s, 16), n)

    def o_send(b):
        o_all[b, orow(dm)] = o_own[b * rb // group:(b + 1) * rb // group].reshape(rb, heads * head).astype(BF16)
        for d in range(2):
            mine = o_all.at[b, orow(dm)]
            go(mine, mine, o_s.at[0, b, d], o_r.at[0, b, d], 'dm', ypeers[d])

    def o_fwd(b):
        for d in range(2):
            got(o_all.at[b, orow(ypeers[1 - d])], o_s.at[0, b, d], o_r.at[0, b, d], 'dm', ypeers[d])
            piece = o_all.at[b, orow(ypeers[1 - d], d * rh, rh)]
            go(piece, piece, o_s.at[1, b, d], o_r.at[1, b, d], 'dm', ypeers[d])

    def o_done(b):
        for d in range(2):
            got(o_all.at[b, orow(far, d * rh, rh)], o_s.at[1, b, d], o_r.at[1, b, d], 'dm', ypeers[d])

    def trow(owner, c, s=0, n=share):
        return pl.ds(al(c * (brows // 2) + owner * share + s, sh), n)

    order = (xf, xn, xp, xi)

    def xs_pair(u, b):
        for i, owner in enumerate(order):
            go(full.at[u, b, trow(owner, 1 - core)], d2d_recv.at[u, b, i], d_s.at[u, b, i], d_r.at[u, b, i], 'tp', partner)

    def xs_ab(u, b):
        for i, owner in enumerate(order):
            got(d2d_recv.at[u, b, i], d_s.at[u, b, i], d_r.at[u, b, i], 'tp', partner)
            here = trow(owner, core)
            full[u, b, here] = full[u, b, here] + d2d_recv[u, b, i]
            if i == 0:
                for d in range(2):
                    go(full.at[u, b, trow(xf, core, d * sh, sh)], xa_recv.at[u, b, d], xa_s.at[u, b, d], xa_r.at[u, b, d], 'tp', xids[d])
            elif i < 3:
                d = i - 1
                go(full.at[u, b, trow(owner, core, (1 - d) * sh, sh)], xb_recv.at[u, b, d], xb_s.at[u, b, d], xb_r.at[u, b, d], 'tp', xids[d])

    def xs_c(u, b):
        for d in range(2):
            got(xa_recv.at[u, b, d], xa_s.at[u, b, d], xa_r.at[u, b, d], 'tp', xids[d])
            xc_send[u, b, d] = xa_recv[u, b, d] + full[u, b, trow(xpeers[d], core, d * sh, sh)]
            go(xc_send.at[u, b, d], xc_recv.at[u, b, d], xc_s.at[u, b, d], xc_r.at[u, b, d], 'tp', xids[d])

    def xs_done(u, b):
        for d in range(2):
            got(xb_recv.at[u, b, d], xb_s.at[u, b, d], xb_r.at[u, b, d], 'tp', xids[d])
            got(xc_recv.at[u, b, d], xc_s.at[u, b, d], xc_r.at[u, b, d], 'tp', xids[d])
        return jnp.concatenate(
            [full[u, b, trow(xi, core, d * sh, sh)] + xc_recv[u, b, d] + xb_recv[u, b, 1 - d] for d in range(2)], axis=0)

    def lanes(d):
        return pl.ds(d * (width // 2), width // 2)

    def ag_send(u, buf, b):
        mine = buf.at[b, trow(xi, core)]
        for d in range(2):
            go(mine, mine, ag_s.at[u, b, d], ag_r.at[u, b, d], 'tp', xids[d])
        go(mine, mine, agd_s.at[u, b, 0], agd_r.at[u, b, 0], 'tp', partner)

    def ag_fwd(u, buf, b):
        for d in range(2):
            near = buf.at[b, trow(xpeers[1 - d], core)]
            got(near, ag_s.at[u, b, d], ag_r.at[u, b, d], 'tp', xids[d])
            piece = buf.at[b, trow(xpeers[1 - d], core), lanes(d)]
            go(piece, piece, agf_s.at[u, b, d], agf_r.at[u, b, d], 'tp', xids[d])
            go(near, near, agd_s.at[u, b, 1 + d], agd_r.at[u, b, 1 + d], 'tp', partner)

    def ag_done(u, buf, b):
        for d in range(2):
            got(buf.at[b, trow(xf, core), lanes(d)], agf_s.at[u, b, d], agf_r.at[u, b, d], 'tp', xids[d])
        last = buf.at[b, trow(xf, core)]
        go(last, last, agd_s.at[u, b, 3], agd_r.at[u, b, 3], 'tp', partner)
        for i, owner in enumerate((xi, xp, xn, xf)):
            got(buf.at[b, trow(owner, 1 - core)], agd_s.at[u, b, i], agd_r.at[u, b, i], 'tp', partner)

    step = 256

    def o_proj(b):
        for n in range(0, width, step):
            full[0, b, :, n:n + step] = jnp.dot(o_all[b], wo[:, n:n + step], preferred_element_type=F32)
        xs_pair(0, b)

    def norm_send(b):
        attn = xs_done(0, b)
        first = trow(xi, core).start
        owner = first // rb
        here = pl.ds(al(owner * rows + b * rb + (first - owner * rb), share), share)
        h1 = h_ref[here] + attn.astype(BF16)
        h1_buf[b] = h1
        h1 = h1.astype(F32)
        col = jnp.sum(h1 * h1, axis=-1, keepdims=True)
        st_send[b] = column_to_row(jnp.concatenate([col] * (128 // share), axis=0))
        for i, peer in enumerate((nxt, prv, far)):
            go(st_send.at[b], st_recv.at[b, i], st_s.at[b, i], st_r.at[b, i], 'dm', peer)

    def norm_done(b):
        for i, peer in enumerate((nxt, prv, far)):
            got(st_recv.at[b, i], st_s.at[b, i], st_r.at[b, i], 'dm', peer)
        total = st_send[b] + st_recv[b, 0] + st_recv[b, 1] + st_recv[b, 2]
        scale = row_to_column(lax.rsqrt(total / width_full + EPS))[:share]
        x2_all[b, trow(xi, core)] = scale_rows(h1_buf[b].astype(F32), scale, g2_ref[...].astype(F32)[None, :])
        ag_send(0, x2_all, b)

    def columns(owner):
        return pl.ds(al(owner * own_cols, 16), own_cols)

    def gu_ab(b):
        for i, owner in enumerate((far, nxt, prv, dm)):
            for j, w in enumerate((wg, wu)):
                y = lax.dot_general(w[columns(owner)], x2_all[b], (((1,), (1,)), ((), ())), preferred_element_type=F32)
                for p in range(PARTS):
                    for s in range(2):
                        gu[b, i, p, s, j] = y[p * pc + s * ph:p * pc + (s + 1) * ph]
            for p in range(PARTS):
                if i == 0:
                    for d in range(2):
                        go(gu.at[b, 0, p, d], ga_recv.at[b, d, p], ga_s.at[b, d, p], ga_r.at[b, d, p], 'dm', ypeers[d])
                elif i < 3:
                    d = i - 1
                    go(gu.at[b, i, p, 1 - d], gb_recv.at[b, d, p], gb_s.at[b, d, p], gb_r.at[b, d, p], 'dm', ypeers[d])

    def gu_c(b):
        for p in range(PARTS):
            for d in range(2):
                got(ga_recv.at[b, d, p], ga_s.at[b, d, p], ga_r.at[b, d, p], 'dm', ypeers[d])
                gc_send[b, d, p] = ga_recv[b, d, p] + gu[b, 1 + d, p, d]
                go(gc_send.at[b, d, p], gc_recv.at[b, d, p], gc_s.at[b, d, p], gc_r.at[b, d, p], 'dm', ypeers[d])

    cut = (pc // 2 + 15) // 16 * 16
    cuts = ((0, cut), (cut, pc - cut))

    def mrow(owner, p, s=0, n=pc):
        return pl.ds(al(owner * own_cols + p * pc + s, 16), n)

    def m_send(b):
        for p in range(PARTS):
            for d in range(2):
                got(gb_recv.at[b, d, p], gb_s.at[b, d, p], gb_r.at[b, d, p], 'dm', ypeers[d])
                got(gc_recv.at[b, d, p], gc_s.at[b, d, p], gc_r.at[b, d, p], 'dm', ypeers[d])
            halves = []
            for d in range(2):
                gate, up = (gu[b, 3, p, d, j] + gc_recv[b, d, p, j] + gb_recv[b, 1 - d, p, j] for j in range(2))
                halves.append(gate * jax.nn.sigmoid(gate) * up)
            m_all[b, mrow(dm, p)] = jnp.concatenate(halves, axis=0).astype(BF16)
            for d in range(2):
                mine = m_all.at[b, mrow(dm, p)]
                go(mine, mine, m_s.at[b, d, p], m_r.at[b, d, p], 'dm', ypeers[d])

    def m_fwd(b):
        for p in range(PARTS):
            for d in range(2):
                got(m_all.at[b, mrow(ypeers[1 - d], p)], m_s.at[b, d, p], m_r.at[b, d, p], 'dm', ypeers[d])
                piece = m_all.at[b, mrow(ypeers[1 - d], p, *cuts[d])]
                go(piece, piece, mf_s.at[b, d, p], mf_r.at[b, d, p], 'dm', ypeers[d])

    def m_done(b):
        for p in range(PARTS):
            for d in range(2):
                got(m_all.at[b, mrow(far, p, *cuts[d])], mf_s.at[b, d, p], mf_r.at[b, d, p], 'dm', ypeers[d])

    def down(b):
        for n in range(0, width, step):
            full[1, b, :, n:n + step] = lax.dot_general(m_all[b], wd[:, n:n + step], (((0,), (0,)), ((), ())), preferred_element_type=F32)
        xs_pair(1, b)

    def h_send(b):
        mlp = xs_done(1, b)
        h_all[b, trow(xi, core)] = h1_buf[b] + mlp.astype(BF16)
        ag_send(1, h_all, b)

    def h_done(b):
        ag_done(1, h_all, b)
        for owner in range(nd):
            out_ref[owner * rows + b * rb:owner * rows + (b + 1) * rb] = h_all[b, owner * rb:(owner + 1) * rb]

    for t in range(3):
        for i in range(heads):
            part[t, :, i * head:(i + 1) * head] = jnp.dot(x_buf[...], wqkv[t, i], preferred_element_type=F32)
        qkv_a(0, t)
        qkv_b(0, t)
    qkv_a(1, 0)
    for t in range(3):
        qkv_c(0, t)
    qkv_a(1, 1)
    qkv_a(1, 2)
    for t in range(3):
        qkv_b(1, t)
    qkv_c(1, 0)
    totals(0)
    loads[7].wait()
    loads[8].wait()
    groups = rb // group
    attention(0, groups)
    o_send(0)
    qkv_c(1, 1)
    qkv_c(1, 2)
    o_fwd(0)
    totals(1)
    o_done(0)
    loads[9].wait()
    o_proj(0)
    attention(groups, groups + groups // 2)
    xs_ab(0, 0)
    attention(groups + groups // 2, 2 * groups)
    o_send(1)
    xs_c(0, 0)
    o_fwd(1)
    loads[10].wait()
    norm_send(0)
    o_done(1)
    o_proj(1)
    norm_done(0)
    xs_ab(0, 1)
    ag_fwd(0, x2_all, 0)
    xs_c(0, 1)
    for load in loads[11:]:
        load.wait()
    ag_done(0, x2_all, 0)
    gu_ab(0)
    norm_send(1)
    gu_c(0)
    norm_done(1)
    ag_fwd(0, x2_all, 1)
    ag_done(0, x2_all, 1)
    gu_ab(1)
    m_send(0)
    gu_c(1)
    m_fwd(0)
    m_done(0)
    down(0)
    xs_ab(1, 0)
    m_send(1)
    xs_c(1, 0)
    m_fwd(1)
    h_send(0)
    m_done(1)
    down(1)
    ag_fwd(1, h_all, 0)
    xs_ab(1, 1)
    xs_c(1, 1)
    h_done(0)
    h_send(1)
    ag_fwd(1, h_all, 1)
    h_done(1)
    for copy in sends:
        copy.wait_send()


def layer(nd, nx, lens, hidden, g1, g2, cos, sin, wq, wk, wv, wo, wg, wu, wd, kc, vc):
    batch, width = hidden.shape
    heads, _, head = wq.shape
    rows, inner, cols = batch // nd, heads * head, wd.shape[0]
    nb = BATCHES
    rh = rows // nb // 2
    brows = batch // nb
    share = brows // (2 * nx)
    vmem = pl.BlockSpec(memory_space=pltpu.VMEM)
    hbm = pl.BlockSpec(memory_space=pl.ANY)
    smem = pl.BlockSpec(memory_space=pltpu.SMEM)
    vm = pltpu.VMEM
    dma = pltpu.SemaphoreType.DMA
    piece = vm((nb, 2, 3, rh, inner), F32)
    xpiece = vm((2, nb, 2, share // 2, width), F32)
    ph = cols // nd // PARTS // 2
    gpiece = vm((nb, 2, PARTS, 2, ph, brows), F32)
    return pl.pallas_call(
        functools.partial(layer_kernel, nd, nx, width * nd),
        out_shape=[jax.ShapeDtypeStruct((batch, width), BF16), jax.ShapeDtypeStruct((rows, inner), F32), jax.ShapeDtypeStruct((rows, inner), F32)],
        in_specs=[smem] + [hbm] * 14,
        out_specs=[vmem] * 3,
        scratch_shapes=[
            vm(hidden.shape, BF16), vm(g1.shape, BF16), vm(g2.shape, BF16), vm(cos.shape, F32), vm(sin.shape, F32),
            vm((3, heads, width, head), BF16), vm(wo.shape, BF16), vm(wg.shape, BF16), vm(wu.shape, BF16), vm(wd.shape, BF16),
            vm(kc.shape, BF16), vm(vc.shape, BF16),
            vm((batch, width), BF16), vm((3, batch, inner), F32), vm((8, batch), F32), vm((3, 8, batch), F32),
            piece, piece, piece, piece, vm((rows, head), F32), vm((rows, head), F32), vm((rows, inner), F32), vm((rows // 8, 8, inner), F32),
            vm((nb, brows, inner), BF16), vm((2, nb, brows, width), F32), vm((2, nb, nx, share, width), F32),
            xpiece, xpiece, xpiece, xpiece, vm((nb, share, width), BF16), vm((nb, 8, 128), F32), vm((nb, 3, 8, 128), F32), vm((nb, brows, width), BF16),
            vm((nb, 4, PARTS, 2, 2, ph, brows), F32), gpiece, gpiece, gpiece, gpiece, vm((nb, cols, brows), BF16), vm((nb, brows, width), BF16),
            dma((14,)), dma((3,)), dma((3,))] + [dma((nb, 2, 3))] * 6 + [dma((2, nb, 2))] * 2 + [dma((2, nb, nx))] * 2 + [dma((2, nb, 2))] * 6
        + [dma((nb, 3))] * 2 + [dma((2, nb, 2))] * 4 + [dma((2, nb, nx))] * 2 + [dma((nb, 2, PARTS))] * 10,
        compiler_params=pltpu.CompilerParams(collective_id=0, has_side_effects=True, vmem_limit_bytes=VMEM_LIMIT),
        name='layer',
    )(lens, hidden, g1, g2, cos, sin, wq, wk, wv, wo, wg, wu, wd, kc, vc)


def update_kernel(lens_ref, kn_ref, vn_ref, h_ref, kc_ref, vc_ref, ko_ref, vo_ref, out_ref):
    step = pl.program_id(0)
    rb, heads, slots, head = kc_ref.shape
    window = 16
    pos = lax.broadcasted_iota(jnp.int32, (heads, window, head), 1)
    out_ref[...] = h_ref[...]
    ko_ref[...] = kc_ref[...]
    vo_ref[...] = vc_ref[...]
    for r in range(rb):
        length = lens_ref[step * rb + r]
        base = pl.multiple_of(length // window * window, window)
        write = pos == length - base
        for new_ref, old, out in ((kn_ref, kc_ref, ko_ref), (vn_ref, vc_ref, vo_ref)):
            new = jnp.stack([jnp.broadcast_to(new_ref[r:r + 1, i * head:(i + 1) * head], (window, head)) for i in range(heads)])
            out[r, :, pl.ds(base, window), :] = jnp.where(write, new, old[r, :, pl.ds(base, window), :].astype(F32)).astype(BF16)


def update(lens, kn, vn, h, kc, vc):
    rows, heads, slots, head = kc.shape
    rb = 8
    steps = rows // rb
    row_block = pl.BlockSpec((rb, heads * head), lambda i, lens: (i, 0))
    h_block = pl.BlockSpec((h.shape[0] // steps, h.shape[1]), lambda i, lens: (i, 0))
    cache_block = pl.BlockSpec((rb, heads, slots, head), lambda i, lens: (i, 0, 0, 0))
    return pl.pallas_call(
        update_kernel,
        grid_spec=pltpu.PrefetchScalarGridSpec(
            num_scalar_prefetch=1, grid=(steps,),
            in_specs=[row_block] * 2 + [h_block] + [cache_block] * 2,
            out_specs=[cache_block, cache_block, h_block]),
        out_shape=[jax.ShapeDtypeStruct(kc.shape, BF16), jax.ShapeDtypeStruct(vc.shape, BF16), jax.ShapeDtypeStruct(h.shape, BF16)],
        compiler_params=pltpu.CompilerParams(vmem_limit_bytes=VMEM_LIMIT),
        name='update',
    )(lens, kn, vn, h, kc, vc)


def solution(mesh):
    nd, nx = mesh.shape['dm'], mesh.shape['tp'] // 2
    row_spec = P('dp', 'dm')
    cache_spec = P(('dp', 'dm'), None, 'tp', None)
    batch_spec = P(('dp', 'dm'))
    rope_spec = P(('dp', 'dm'), None)
    in_specs = (row_spec, P('dm', 'tp', None), P('dm', 'tp', None), P('dm', 'tp', None), P('tp', None, 'dm'), P('dm', 'tp'), P('dm', 'tp'), P('tp', 'dm'), P('dm'), P('dm'), cache_spec, cache_spec, batch_spec, rope_spec, rope_spec)
    out_specs = (row_spec, cache_spec, cache_spec)

    def local_layer(hidden, w_q, w_k, w_v, w_o, w_gate, w_up, w_down, norm_attn, norm_mlp, k_cache, v_cache, seq_lens, rope_cos, rope_sin):
        wq, wk, wv = (w.transpose(1, 0, 2) for w in (w_q, w_k, w_v))
        kc, vc = (c.transpose(0, 2, 1, 3) for c in (k_cache, v_cache))
        h_out, kn, vn = layer(nd, nx, seq_lens, hidden, norm_attn, norm_mlp, rope_cos, rope_sin, wq, wk, wv, w_o.reshape(-1, w_o.shape[-1]), w_gate.T, w_up.T, w_down, kc, vc)
        ko, vo, h_out = update(seq_lens, kn, vn, h_out, kc, vc)
        return h_out, ko.transpose(0, 2, 1, 3), vo.transpose(0, 2, 1, 3)

    return jax.shard_map(local_layer, mesh=mesh, in_specs=in_specs, out_specs=out_specs, check_vma=False)
```

```python
import functools

import jax
import jax.numpy as jnp
from jax import lax
from jax.experimental import pallas as pl
from jax.experimental.pallas import tpu as pltpu
from jax.sharding import PartitionSpec as P

EPS = 1e-6
F32 = jnp.float32
BF16 = jnp.bfloat16
MESH = pl.DeviceIdType.MESH
VMEM_LIMIT = 63 * 2 ** 20
BATCHES = 2
UPDATE_CHUNKS = 8
PARTS = 3


def remote(src, dst, send, recv, axis, index):
    return pltpu.make_async_remote_copy(
        src_ref=src, dst_ref=dst, send_sem=send, recv_sem=recv, device_id={axis: index}, device_id_type=MESH)


def entry_barrier(peers):
    barrier = pltpu.get_barrier_semaphore()
    for axis, index in peers:
        pl.semaphore_signal(barrier, inc=1, device_id={axis: index}, device_id_type=MESH)
    return lambda: pl.semaphore_wait(barrier, len(peers))


def column_to_row(col):
    rows = col.shape[0]
    return jnp.concatenate(
        [jnp.broadcast_to(col[i:i + 128], (128, 128)).T[:8] for i in range(0, rows, 128)], axis=1)


def row_to_column(row):
    rows = row.shape[1]
    return jnp.concatenate(
        [jnp.broadcast_to(row[:1, i:i + 128], (128, 128)).T for i in range(0, rows, 128)], axis=0)


def scale_rows(x, scale, gain):
    width = x.shape[1]
    cols = [x[:, i:i + 128] * scale * gain[:, i:i + 128] for i in range(0, width, 128)]
    return jnp.concatenate(cols, axis=1).astype(BF16)


def layer_kernel(nd, nx, width_full, lens_hbm, h_hbm, g1_hbm, g2_hbm, cos_hbm, sin_hbm, wq_hbm, wk_hbm, wv_hbm, wo_hbm, wg_hbm, wu_hbm, wd_hbm,
                 kc_hbm, vc_hbm, out_ref, k_out, v_out, lens_smem,
                 h_ref, g1_ref, g2_ref, cos_ref, sin_ref, wqkv, wo, wg, wu, wd, kc, vc,
                 x_buf, part, ss_send, ss_recv, a_recv, b_recv, c_send, c_recv, cos2, sin2, q_buf, o_own,
                 o_all, full, d2d_recv, xs_recv, h1_all, st_col, st_send, st_recv, sc_send, sc_recv, x2_all,
                 gu, ga_recv, gb_recv, gc_send, gc_recv, m_all, h_all,
                 w_sem, ss_s, ss_r, a_s, a_r, b_s, b_r, c_s, c_r, o_s, o_r, d_s, d_r, xs_s, xs_r,
                 st_s, st_r, sc_s, sc_r, ag_s, ag_r, agd_s, agd_r, ga_s, ga_r, gb_s, gb_r, gc_s, gc_r, m_s, m_r, mf_s, mf_r):
    dm, tp = lax.axis_index('dm'), lax.axis_index('tp')
    nxt, prv, far = lax.rem(dm + 1, nd), lax.rem(dm + nd - 1, nd), lax.rem(dm + 2, nd)
    core, xi = lax.rem(tp, 2), tp // 2
    xn, xp, xf = lax.rem(xi + 1, nx), lax.rem(xi + nx - 1, nx), lax.rem(xi + 2, nx)
    partner = tp + 1 - 2 * core
    ypeers, yall = (nxt, prv), (far, nxt, prv)
    xall = (xf, xn, xp)
    xids = tuple(2 * x + core for x in xall)
    source = (0, 2, 1)
    batch, width = h_ref.shape
    heads, slots, head = kc.shape[1:]
    rows = batch // nd
    rb = rows // BATCHES
    rh = rb // 2
    brows = nd * rb
    share = brows // (2 * nx)
    sh = share // 2
    cols = wd.shape[0]
    own_cols = cols // nd
    pc = own_cols // PARTS
    ph = pc // 2
    sends = []

    def go(*args):
        sends.append(remote(*args))
        sends[-1].start()

    def got(ref, send, recv, axis, index):
        remote(ref, ref, send, recv, axis, index).wait_recv()

    def al(x, n):
        return pl.multiple_of(x, n)

    wait_barrier = entry_barrier([('dm', y) for y in yall] + [('tp', lax.rem(tp + i, 2 * nx)) for i in range(1, 2 * nx)])
    pairs = ((h_hbm, h_ref), (wq_hbm, wqkv.at[0]), (wk_hbm, wqkv.at[1]), (wv_hbm, wqkv.at[2]), (g1_hbm, g1_ref), (cos_hbm, cos_ref), (sin_hbm, sin_ref),
             (kc_hbm, kc), (vc_hbm, vc), (wo_hbm, wo), (g2_hbm, g2_ref), (wg_hbm, wg), (wu_hbm, wu), (wd_hbm, wd))
    loads = [pltpu.make_async_copy(src, dst, w_sem.at[i]) for i, (src, dst) in enumerate(pairs)]
    loads[0].start()
    for load in loads[4:7]:
        load.start()
    loads[0].wait()
    for load in loads[1:4]:
        load.start()
    lens_load = pltpu.make_async_copy(lens_hbm, lens_smem, w_sem.at[14])
    lens_load.start()
    st_col[...] = jnp.zeros_like(st_col)
    x = h_ref[...].astype(F32)
    ss_send[...] = column_to_row(jnp.sum(x * x, axis=-1, keepdims=True))
    wait_barrier()
    for i, peer in enumerate((nxt, prv, far)):
        go(ss_send, ss_recv.at[i], ss_s.at[i], ss_r.at[i], 'dm', peer)
    for load in loads[4:7]:
        load.wait()
    hd = cos_ref.shape[1]
    cos2[:, :hd] = cos_ref[...]
    cos2[:, hd:] = cos_ref[...]
    sin2[:, :hd] = -sin_ref[...]
    sin2[:, hd:] = sin_ref[...]
    for i, peer in enumerate((nxt, prv, far)):
        got(ss_recv.at[i], ss_s.at[i], ss_r.at[i], 'dm', peer)
    for load in loads[7:]:
        load.start()
    total = ss_send[...] + ss_recv[0] + ss_recv[1] + ss_recv[2]
    scale = row_to_column(lax.rsqrt(total / width_full + EPS))
    x_buf[...] = scale_rows(h_ref[...].astype(F32), scale, g1_ref[...].astype(F32)[None, :])

    def prow(owner, b, s):
        return pl.ds(al(owner * rows + b * rb + s * rh, rh), rh)

    def qkv_a(b, t):
        for d in range(2):
            go(part.at[t, prow(far, b, d)], a_recv.at[b, d, t], a_s.at[b, d, t], a_r.at[b, d, t], 'dm', ypeers[d])

    def qkv_b(b, t):
        for d in range(2):
            go(part.at[t, prow(ypeers[d], b, 1 - d)], b_recv.at[b, d, t], b_s.at[b, d, t], b_r.at[b, d, t], 'dm', ypeers[d])

    def qkv_c(b, t):
        for d in range(2):
            got(a_recv.at[b, d, t], a_s.at[b, d, t], a_r.at[b, d, t], 'dm', ypeers[d])
            c_send[b, d, t] = a_recv[b, d, t] + part[t, prow(ypeers[d], b, d)]
            go(c_send.at[b, d, t], c_recv.at[b, d, t], c_s.at[b, d, t], c_r.at[b, d, t], 'dm', ypeers[d])

    def totals(b):
        for t, out in enumerate((q_buf, k_out, v_out)):
            for d in range(2):
                got(b_recv.at[b, d, t], b_s.at[b, d, t], b_r.at[b, d, t], 'dm', ypeers[d])
                got(c_recv.at[b, d, t], c_s.at[b, d, t], c_r.at[b, d, t], 'dm', ypeers[d])
            for d in range(2):
                tot = part[t, prow(dm, b, d)] + c_recv[b, d, t] + b_recv[b, 1 - d, t]
                here = slice(b * rb + d * rh, b * rb + (d + 1) * rh)
                for i in range(heads):
                    y = tot[:, i * head:(i + 1) * head]
                    if t < 2:
                        y = y * cos2[here] + pltpu.roll(y, head // 2, 1) * sin2[here]
                    out[here, i * head:(i + 1) * head] = y.astype(BF16).astype(F32)

    span = heads * slots
    group = 8

    def attention(lo, hi):
        lane = lax.broadcasted_iota(jnp.int32, (8, span), 1)
        lane_slot = lane % slots
        own_head = (lane // slots) == lax.broadcasted_iota(jnp.int32, (8, span), 0)
        head_row = lax.broadcasted_iota(jnp.int32, (8, head), 0)

        def body(g, carry):
            first = al(g * group, group)
            vals = [ref[pl.ds(first, group), :] for ref in (q_buf, k_out, v_out)]

            def per_head(val, r):
                y = jnp.zeros((8, head), F32)
                for i in range(heads):
                    y = jnp.where(head_row == i, jnp.broadcast_to(val[r:r + 1, i * head:(i + 1) * head], (8, head)), y)
                return y

            scores, masks, news = [], [], []
            for r in range(group):
                q = per_head(vals[0], r)
                k = kc[first + r].reshape(span, head)
                s = lax.dot_general(q.astype(BF16), k, (((1,), (1,)), ((), ())), preferred_element_type=F32)
                masks.append(own_head & (lane_slot < lens_smem[first + r]))
                scores.append(jnp.where(masks[r], s * (head ** -0.5), float(jnp.finfo(F32).min)))
                news.append(jnp.sum(q * per_head(vals[1], r), axis=-1, keepdims=True) * (head ** -0.5))
            s, new = jnp.stack(scores), jnp.stack(news)
            top = jnp.maximum(jnp.max(s, axis=-1, keepdims=True), new)
            p = jnp.where(jnp.stack(masks), jnp.exp(s - top), 0.0)
            p_new = jnp.exp(new - top)
            den = jnp.sum(p, axis=-1, keepdims=True) + p_new
            p = (p / den).astype(BF16)
            p_new = (p_new / den).astype(BF16).astype(F32)
            for r in range(group):
                o = jnp.dot(p[r], vc[first + r].reshape(span, head), preferred_element_type=F32) + p_new[r] * per_head(vals[2], r)
                for i in range(heads):
                    o_own[g, r:r + 1, i * head:(i + 1) * head] = o[i:i + 1]
            return carry

        lax.fori_loop(lo, hi, body, 0)

    def orow(owner, s=0, n=rb):
        return pl.ds(al(owner * rb + s, 16), n)

    def o_send(b):
        o_all[b, orow(dm)] = o_own[b * rb // group:(b + 1) * rb // group].reshape(rb, heads * head).astype(BF16)
        mine = o_all.at[b, orow(dm)]
        for k, peer in enumerate(yall):
            go(mine, mine, o_s.at[b, k], o_r.at[b, k], 'dm', peer)

    def o_done(b):
        for k, peer in enumerate(yall):
            got(o_all.at[b, orow(yall[source[k]])], o_s.at[b, k], o_r.at[b, k], 'dm', peer)

    def trow(owner, c, s=0, n=share):
        return pl.ds(al(c * (brows // 2) + owner * share + s, sh), n)

    order = (xf, xn, xp, xi)

    def xs_pair(u, b):
        for i, owner in enumerate(order):
            go(full.at[u, b, trow(owner, 1 - core)], d2d_recv.at[u, b, i], d_s.at[u, b, i], d_r.at[u, b, i], 'tp', partner)

    def xs_ab(u, b):
        for i, owner in enumerate(order):
            got(d2d_recv.at[u, b, i], d_s.at[u, b, i], d_r.at[u, b, i], 'tp', partner)
            here = trow(owner, core)
            full[u, b, here] = full[u, b, here] + d2d_recv[u, b, i]
            if i < 3:
                go(full.at[u, b, here], xs_recv.at[u, b, i], xs_s.at[u, b, i], xs_r.at[u, b, i], 'tp', xids[i])

    def xs_done(u, b):
        for i in range(3):
            got(xs_recv.at[u, b, i], xs_s.at[u, b, i], xs_r.at[u, b, i], 'tp', xids[i])
        return (full[u, b, trow(xi, core)] + xs_recv[u, b, 0]) + (xs_recv[u, b, 1] + xs_recv[u, b, 2])

    def ag_send(u, buf, b):
        mine = buf.at[b, trow(xi, core)]
        for k in range(3):
            go(mine, mine, ag_s.at[u, b, k], ag_r.at[u, b, k], 'tp', xids[k])
        go(mine, mine, agd_s.at[u, b, 3], agd_r.at[u, b, 3], 'tp', partner)

    def ag_fwd(u, buf, b):
        for k in (1, 2, 0):
            came = buf.at[b, trow(xall[source[k]], core)]
            got(came, ag_s.at[u, b, k], ag_r.at[u, b, k], 'tp', xids[k])
            go(came, came, agd_s.at[u, b, k], agd_r.at[u, b, k], 'tp', partner)

    def ag_done(u, buf, b):
        for k in range(3):
            got(buf.at[b, trow(xall[source[k]], 1 - core)], agd_s.at[u, b, k], agd_r.at[u, b, k], 'tp', partner)
        got(buf.at[b, trow(xi, 1 - core)], agd_s.at[u, b, 3], agd_r.at[u, b, 3], 'tp', partner)

    step = 256

    def o_proj(b):
        o_done(b)
        need(9)
        for n in range(0, width, step):
            full[0, b, :, n:n + step] = jnp.dot(o_all[b], wo[:, n:n + step], preferred_element_type=F32)
        xs_pair(0, b)

    def norm_send(b):
        attn = xs_done(0, b)
        first = trow(xi, core).start
        owner = first // rb
        here = pl.ds(al(owner * rows + b * rb + (first - owner * rb), share), share)
        h1 = h_ref[here] + attn.astype(BF16)
        h1_all[b, trow(xi, core)] = h1
        ag_send(0, h1_all, b)
        h1 = h1.astype(F32)
        col = jnp.sum(h1 * h1, axis=-1, keepdims=True)
        st_col[b, trow(xi, core)] = jnp.broadcast_to(col, (share, 128))
        st_send[b] = st_col[b].T[:8]
        for k, peer in enumerate(yall):
            go(st_send.at[b], st_recv.at[b, k], st_s.at[b, k], st_r.at[b, k], 'dm', peer)

    def norm_mid(b):
        for k, peer in enumerate(yall):
            got(st_recv.at[b, k], st_s.at[b, k], st_r.at[b, k], 'dm', peer)
        sc_send[b] = st_send[b] + st_recv[b, 0] + st_recv[b, 1] + st_recv[b, 2]
        for i in range(2 * nx - 1):
            go(sc_send.at[b], sc_recv.at[b, i], sc_s.at[b, i], sc_r.at[b, i], 'tp', lax.rem(tp + i + 1, 2 * nx))

    def norm_done(b):
        total = sc_send[b]
        for i in range(2 * nx - 1):
            got(sc_recv.at[b, i], sc_s.at[b, i], sc_r.at[b, i], 'tp', lax.rem(tp + i + 1, 2 * nx))
            total = total + sc_recv[b, i]
        ag_done(0, h1_all, b)
        need(10)
        scale = row_to_column(lax.rsqrt(total / width_full + EPS))
        x2_all[b] = scale_rows(h1_all[b].astype(F32), scale, g2_ref[...].astype(F32)[None, :])

    def columns(owner):
        return pl.ds(al(owner * own_cols, 16), own_cols)

    def gu_part(b, i):
        need(11, 12)
        for j, w in enumerate((wg, wu)):
            y = lax.dot_general(w[columns((far, nxt, prv, dm)[i])], x2_all[b], (((1,), (1,)), ((), ())), preferred_element_type=F32)
            for p in range(PARTS):
                for s in range(2):
                    gu[b, i, p, s, j] = y[p * pc + s * ph:p * pc + (s + 1) * ph]
        for p in range(PARTS):
            if i == 0:
                for d in range(2):
                    go(gu.at[b, 0, p, d], ga_recv.at[b, d, p], ga_s.at[b, d, p], ga_r.at[b, d, p], 'dm', ypeers[d])
            elif i < 3:
                d = i - 1
                go(gu.at[b, i, p, 1 - d], gb_recv.at[b, d, p], gb_s.at[b, d, p], gb_r.at[b, d, p], 'dm', ypeers[d])

    def gu_c(b, p):
        for d in range(2):
            got(ga_recv.at[b, d, p], ga_s.at[b, d, p], ga_r.at[b, d, p], 'dm', ypeers[d])
            gc_send[b, d, p] = ga_recv[b, d, p] + gu[b, 1 + d, p, d]
            go(gc_send.at[b, d, p], gc_recv.at[b, d, p], gc_s.at[b, d, p], gc_r.at[b, d, p], 'dm', ypeers[d])

    cut = (pc // 2 + 15) // 16 * 16
    cuts = ((0, cut), (cut, pc - cut))

    def mrow(owner, p, s=0, n=pc):
        return pl.ds(al(owner * own_cols + p * pc + s, 16), n)

    def straight(b):
        return b == BATCHES - 1

    def m_send(b, p):
        for d in range(2):
            got(gb_recv.at[b, d, p], gb_s.at[b, d, p], gb_r.at[b, d, p], 'dm', ypeers[d])
            got(gc_recv.at[b, d, p], gc_s.at[b, d, p], gc_r.at[b, d, p], 'dm', ypeers[d])
        halves = []
        for d in range(2):
            gate, up = (gu[b, 3, p, d, j] + gc_recv[b, d, p, j] + gb_recv[b, 1 - d, p, j] for j in range(2))
            halves.append(gate * jax.nn.sigmoid(gate) * up)
        m_all[b, mrow(dm, p)] = jnp.concatenate(halves, axis=0).astype(BF16)
        mine = m_all.at[b, mrow(dm, p)]
        if straight(b):
            go(mine, mine, mf_s.at[b, 0, p], mf_r.at[b, 0, p], 'dm', far)
        for d in range(2):
            go(mine, mine, m_s.at[b, d, p], m_r.at[b, d, p], 'dm', ypeers[d])

    def m_fwd(b, p):
        for d in range(2):
            got(m_all.at[b, mrow(ypeers[1 - d], p)], m_s.at[b, d, p], m_r.at[b, d, p], 'dm', ypeers[d])
            if not straight(b):
                piece = m_all.at[b, mrow(ypeers[1 - d], p, *cuts[d])]
                go(piece, piece, mf_s.at[b, d, p], mf_r.at[b, d, p], 'dm', ypeers[d])

    def m_done(b):
        for p in range(PARTS):
            if straight(b):
                got(m_all.at[b, mrow(far, p)], mf_s.at[b, 0, p], mf_r.at[b, 0, p], 'dm', far)
            else:
                for d in range(2):
                    got(m_all.at[b, mrow(far, p, *cuts[d])], mf_s.at[b, d, p], mf_r.at[b, d, p], 'dm', ypeers[d])

    def down(b):
        m_done(b)
        need(13)
        for n in range(0, width, step):
            full[1, b, :, n:n + step] = lax.dot_general(m_all[b], wd[:, n:n + step], (((0,), (0,)), ((), ())), preferred_element_type=F32)
        xs_pair(1, b)

    def h_send(b):
        mlp = xs_done(1, b)
        h_all[b, trow(xi, core)] = h1_all[b, trow(xi, core)] + mlp.astype(BF16)
        ag_send(1, h_all, b)

    def h_done(b):
        ag_done(1, h_all, b)
        for owner in range(nd):
            out_ref[owner * rows + b * rb:owner * rows + (b + 1) * rb] = h_all[b, owner * rb:(owner + 1) * rb]

    waited = set()

    def need(*which):
        for i in which:
            if i not in waited:
                waited.add(i)
                loads[i].wait()

    def mm(t):
        need(1 + t)
        for i in range(heads):
            part[t, :, i * head:(i + 1) * head] = jnp.dot(x_buf[...], wqkv[t, i], preferred_element_type=F32)

    mm(0)
    qkv_a(0, 0)
    qkv_b(0, 0)
    mm(1)
    mm(2)
    qkv_a(0, 1)
    qkv_a(0, 2)
    qkv_a(1, 0)
    qkv_b(0, 2)
    qkv_b(0, 1)
    qkv_a(1, 1)
    qkv_c(0, 0)
    qkv_a(1, 2)
    qkv_c(0, 1)
    qkv_c(0, 2)
    qkv_c(1, 0)
    qkv_b(1, 0)
    qkv_c(1, 1)
    qkv_b(1, 2)
    qkv_c(1, 2)
    qkv_b(1, 1)
    totals(0)
    need(7, 8)
    lens_load.wait()
    attention(2, 4)
    attention(0, 2)
    o_send(0)
    totals(1)
    attention(6, 8)
    attention(4, 6)
    o_send(1)
    o_proj(0)
    xs_ab(0, 0)
    o_proj(1)
    xs_ab(0, 1)
    norm_send(0)
    norm_mid(0)
    norm_send(1)
    ag_fwd(0, h1_all, 0)
    norm_done(0)
    gu_part(0, 0)
    norm_mid(1)
    ag_fwd(0, h1_all, 1)
    gu_part(0, 1)
    norm_done(1)
    gu_part(1, 0)
    gu_part(0, 2)
    gu_part(0, 3)
    gu_c(0, 0)
    gu_c(0, 1)
    gu_c(0, 2)
    gu_part(1, 1)
    m_send(0, 0)
    m_send(0, 1)
    m_send(0, 2)
    gu_part(1, 2)
    gu_part(1, 3)
    gu_c(1, 1)
    gu_c(1, 2)
    gu_c(1, 0)
    m_fwd(0, 0)
    m_fwd(0, 1)
    m_fwd(0, 2)
    m_send(1, 1)
    m_send(1, 2)
    m_send(1, 0)
    down(0)
    m_fwd(1, 1)
    xs_ab(1, 0)
    m_fwd(1, 2)
    m_fwd(1, 0)
    down(1)
    xs_ab(1, 1)
    h_send(0)
    h_send(1)
    ag_fwd(1, h_all, 0)
    h_done(0)
    ag_fwd(1, h_all, 1)
    h_done(1)
    for copy in sends:
        copy.wait_send()


def layer(nd, nx, lens, hidden, g1, g2, cos, sin, wq, wk, wv, wo, wg, wu, wd, kc, vc):
    batch, width = hidden.shape
    heads, _, head = wq.shape
    rows, inner, cols = batch // nd, heads * head, wd.shape[0]
    nb = BATCHES
    rh = rows // nb // 2
    brows = batch // nb
    share = brows // (2 * nx)
    vmem = pl.BlockSpec(memory_space=pltpu.VMEM)
    hbm = pl.BlockSpec(memory_space=pl.ANY)
    vm = pltpu.VMEM
    dma = pltpu.SemaphoreType.DMA
    piece = vm((nb, 2, 3, rh, inner), F32)
    ph = cols // nd // PARTS // 2
    gpiece = vm((nb, 2, PARTS, 2, ph, brows), F32)
    return pl.pallas_call(
        functools.partial(layer_kernel, nd, nx, width * nd),
        out_shape=[jax.ShapeDtypeStruct((batch, width), BF16), jax.ShapeDtypeStruct((rows, inner), F32), jax.ShapeDtypeStruct((rows, inner), F32)],
        in_specs=[hbm] * 15,
        out_specs=[vmem] * 3,
        scratch_shapes=[
            pltpu.SMEM(lens.shape, jnp.int32), vm(hidden.shape, BF16), vm(g1.shape, BF16), vm(g2.shape, BF16), vm(cos.shape, F32), vm(sin.shape, F32),
            vm((3, heads, width, head), BF16), vm(wo.shape, BF16), vm(wg.shape, BF16), vm(wu.shape, BF16), vm(wd.shape, BF16),
            vm(kc.shape, BF16), vm(vc.shape, BF16),
            vm((batch, width), BF16), vm((3, batch, inner), F32), vm((8, batch), F32), vm((3, 8, batch), F32),
            piece, piece, piece, piece, vm((rows, head), F32), vm((rows, head), F32), vm((rows, inner), F32), vm((rows // 8, 8, inner), F32),
            vm((nb, brows, inner), BF16), vm((2, nb, brows, width), F32), vm((2, nb, nx, share, width), F32),
            vm((2, nb, 3, share, width), F32), vm((nb, brows, width), BF16), vm((nb, brows, 128), F32), vm((nb, 8, brows), F32), vm((nb, 3, 8, brows), F32),
            vm((nb, 8, brows), F32), vm((nb, 2 * nx - 1, 8, brows), F32), vm((nb, brows, width), BF16),
            vm((nb, 4, PARTS, 2, 2, ph, brows), F32), gpiece, gpiece, gpiece, gpiece, vm((nb, cols, brows), BF16), vm((nb, brows, width), BF16),
            dma((15,)), dma((3,)), dma((3,))] + [dma((nb, 2, 3))] * 6 + [dma((nb, 3))] * 2 + [dma((2, nb, nx))] * 2 + [dma((2, nb, 3))] * 2
        + [dma((nb, 3))] * 2 + [dma((nb, 2 * nx - 1))] * 2 + [dma((2, nb, 3))] * 2 + [dma((2, nb, nx))] * 2 + [dma((nb, 2, PARTS))] * 10,
        compiler_params=pltpu.CompilerParams(collective_id=0, has_side_effects=True, vmem_limit_bytes=VMEM_LIMIT),
        name='layer',
    )(lens, hidden, g1, g2, cos, sin, wq, wk, wv, wo, wg, wu, wd, kc, vc)


def update_kernel(lens_ref, kn_ref, vn_ref, h_hbm, kc_hbm, vc_hbm, ko_hbm, vo_hbm, out_hbm, kc, vc, h_buf, in_sem, out_sem):
    rows, heads, slots, head = kc.shape
    chunk = rows // UPDATE_CHUNKS
    window = 16
    pos = lax.broadcasted_iota(jnp.int32, (heads, window, head), 1)

    def copies(c):
        here = pl.ds(c * chunk, chunk)
        return [(pltpu.make_async_copy(src.at[here], buf.at[here], in_sem.at[i, c]), pltpu.make_async_copy(buf.at[here], dst.at[here], out_sem.at[i, c]))
                for i, (src, buf, dst) in enumerate(((kc_hbm, kc, ko_hbm), (vc_hbm, vc, vo_hbm)))]

    h_in = pltpu.make_async_copy(h_hbm, h_buf, in_sem.at[2, 0])
    h_out = pltpu.make_async_copy(h_buf, out_hbm, out_sem.at[2, 0])
    for c in range(UPDATE_CHUNKS):
        for load, _ in copies(c):
            load.start()
    h_in.start()

    def body(c, carry):
        pairs = copies(c)
        for load, _ in pairs:
            load.wait()
        first = pl.multiple_of(c * chunk, chunk)
        new_all = [ref[pl.ds(first, chunk), :] for ref in (kn_ref, vn_ref)]
        for r in range(chunk):
            length = lens_ref[first + r]
            base = pl.multiple_of(length // window * window, window)
            write = pos == length - base
            for vals, buf in zip(new_all, (kc, vc)):
                new = jnp.stack([jnp.broadcast_to(vals[r:r + 1, i * head:(i + 1) * head], (window, head)) for i in range(heads)])
                old = buf[first + r, :, pl.ds(base, window), :]
                buf[first + r, :, pl.ds(base, window), :] = jnp.where(write, new, old.astype(F32)).astype(BF16)
        for _, store in pairs:
            store.start()
        return carry

    lax.fori_loop(0, UPDATE_CHUNKS, body, 0)
    h_in.wait()
    h_out.start()
    for c in range(UPDATE_CHUNKS):
        for _, store in copies(c):
            store.wait()
    h_out.wait()


def update(lens, kn, vn, h, kc, vc):
    smem = pl.BlockSpec(memory_space=pltpu.SMEM)
    vmem = pl.BlockSpec(memory_space=pltpu.VMEM)
    hbm = pl.BlockSpec(memory_space=pl.ANY)
    dma = pltpu.SemaphoreType.DMA
    return pl.pallas_call(
        update_kernel,
        in_specs=[smem, vmem, vmem, hbm, hbm, hbm],
        out_specs=[hbm] * 3,
        out_shape=[jax.ShapeDtypeStruct(kc.shape, BF16), jax.ShapeDtypeStruct(vc.shape, BF16), jax.ShapeDtypeStruct(h.shape, BF16)],
        scratch_shapes=[pltpu.VMEM(kc.shape, BF16), pltpu.VMEM(vc.shape, BF16), pltpu.VMEM(h.shape, BF16),
                        dma((3, UPDATE_CHUNKS)), dma((3, UPDATE_CHUNKS))],
        compiler_params=pltpu.CompilerParams(vmem_limit_bytes=VMEM_LIMIT),
        name='update',
    )(lens, kn, vn, h, kc, vc)


def solution(mesh):
    nd, nx = mesh.shape['dm'], mesh.shape['tp'] // 2
    row_spec = P('dp', 'dm')
    cache_spec = P(('dp', 'dm'), None, 'tp', None)
    batch_spec = P(('dp', 'dm'))
    rope_spec = P(('dp', 'dm'), None)
    in_specs = (row_spec, P('dm', 'tp', None), P('dm', 'tp', None), P('dm', 'tp', None), P('tp', None, 'dm'), P('dm', 'tp'), P('dm', 'tp'), P('tp', 'dm'), P('dm'), P('dm'), cache_spec, cache_spec, batch_spec, rope_spec, rope_spec)
    out_specs = (row_spec, cache_spec, cache_spec)

    def local_layer(hidden, w_q, w_k, w_v, w_o, w_gate, w_up, w_down, norm_attn, norm_mlp, k_cache, v_cache, seq_lens, rope_cos, rope_sin):
        wq, wk, wv = (w.transpose(1, 0, 2) for w in (w_q, w_k, w_v))
        kc, vc = (c.transpose(0, 2, 1, 3) for c in (k_cache, v_cache))
        h_out, kn, vn = layer(nd, nx, seq_lens, hidden, norm_attn, norm_mlp, rope_cos, rope_sin, wq, wk, wv, w_o.reshape(-1, w_o.shape[-1]), w_gate.T, w_up.T, w_down, kc, vc)
        ko, vo, h_out = update(seq_lens, kn, vn, h_out, kc, vc)
        return h_out, ko.transpose(0, 2, 1, 3), vo.transpose(0, 2, 1, 3)

    return jax.shard_map(local_layer, mesh=mesh, in_specs=in_specs, out_specs=out_specs, check_vma=False)
```

```python
import functools

import jax
import jax.numpy as jnp
from jax import lax
from jax.experimental import pallas as pl
from jax.experimental.pallas import tpu as pltpu
from jax.sharding import PartitionSpec as P

EPS = 1e-6
F32 = jnp.float32
BF16 = jnp.bfloat16
MESH = pl.DeviceIdType.MESH
LAYER_VMEM = 52 * 2 ** 20
UPDATE_VMEM = 16 * 2 ** 20
BATCHES = 2
UPDATE_CHUNKS = 8
PARTS = 3


def remote(src, dst, send, recv, axis, index):
    return pltpu.make_async_remote_copy(
        src_ref=src, dst_ref=dst, send_sem=send, recv_sem=recv, device_id={axis: index}, device_id_type=MESH)


def entry_barrier(peers):
    barrier = pltpu.get_barrier_semaphore()
    for axis, index in peers:
        pl.semaphore_signal(barrier, inc=1, device_id={axis: index}, device_id_type=MESH)
    return lambda: pl.semaphore_wait(barrier, len(peers))


def column_to_row(col):
    rows = col.shape[0]
    return jnp.concatenate(
        [jnp.broadcast_to(col[i:i + 128], (128, 128)).T[:8] for i in range(0, rows, 128)], axis=1)


def row_to_column(row):
    rows = row.shape[1]
    return jnp.concatenate(
        [jnp.broadcast_to(row[:1, i:i + 128], (128, 128)).T for i in range(0, rows, 128)], axis=0)


def scale_rows(x, scale, gain):
    width = x.shape[1]
    cols = [x[:, i:i + 128] * scale * gain[:, i:i + 128] for i in range(0, width, 128)]
    return jnp.concatenate(cols, axis=1).astype(BF16)


def layer_kernel(nd, nx, width_full, lens_hbm, h_hbm, g1_hbm, g2_hbm, cos_hbm, sin_hbm, wq_hbm, wk_hbm, wv_hbm, wo_hbm, wg_hbm, wu_hbm, wd_hbm,
                 kc_hbm, vc_hbm, out_ref, k_out, v_out, kc, vc, lens_smem,
                 h_ref, g1_ref, g2_ref, cos_ref, sin_ref, wqkv, wo, wg, wu, wd,
                 x_buf, part, ss_send, ss_recv, a_recv, b_recv, c_send, c_recv, cos2, sin2, q_buf, o_own,
                 o_all, full, d2d_recv, xs_recv, h1_all, st_col, st_send, st_recv, sc_send, sc_recv, x2_all,
                 gu, ga_recv, gb_recv, gc_send, gc_recv, m_all, h_all,
                 w_sem, ss_s, ss_r, a_s, a_r, b_s, b_r, c_s, c_r, o_s, o_r, d_s, d_r, xs_s, xs_r,
                 st_s, st_r, sc_s, sc_r, ag_s, ag_r, agd_s, agd_r, ga_s, ga_r, gb_s, gb_r, gc_s, gc_r, m_s, m_r, mf_s, mf_r):
    dm, tp = lax.axis_index('dm'), lax.axis_index('tp')
    nxt, prv, far = lax.rem(dm + 1, nd), lax.rem(dm + nd - 1, nd), lax.rem(dm + 2, nd)
    core, xi = lax.rem(tp, 2), tp // 2
    xn, xp, xf = lax.rem(xi + 1, nx), lax.rem(xi + nx - 1, nx), lax.rem(xi + 2, nx)
    partner = tp + 1 - 2 * core
    ypeers, yall = (nxt, prv), (far, nxt, prv)
    xall = (xf, xn, xp)
    xids = tuple(2 * x + core for x in xall)
    source = (0, 2, 1)
    batch, width = h_ref.shape
    heads, slots, head = kc.shape[1:]
    rows = batch // nd
    rb = rows // BATCHES
    rh = rb // 2
    brows = nd * rb
    share = brows // (2 * nx)
    sh = share // 2
    cols = wd.shape[0]
    own_cols = cols // nd
    pc = own_cols // PARTS
    ph = pc // 2
    sends = []

    def go(*args):
        sends.append(remote(*args))
        sends[-1].start()

    def got(ref, send, recv, axis, index):
        remote(ref, ref, send, recv, axis, index).wait_recv()

    def al(x, n):
        return pl.multiple_of(x, n)

    wait_barrier = entry_barrier([('dm', y) for y in yall] + [('tp', lax.rem(tp + i, 2 * nx)) for i in range(1, 2 * nx)])
    pairs = ((h_hbm, h_ref), (wq_hbm, wqkv.at[0]), (wk_hbm, wqkv.at[1]), (wv_hbm, wqkv.at[2]), (g1_hbm, g1_ref), (cos_hbm, cos_ref), (sin_hbm, sin_ref),
             (kc_hbm, kc), (vc_hbm, vc), (wo_hbm, wo), (g2_hbm, g2_ref), (wg_hbm, wg), (wu_hbm, wu), (wd_hbm, wd))
    loads = [pltpu.make_async_copy(src, dst, w_sem.at[i]) for i, (src, dst) in enumerate(pairs)]
    loads[0].start()
    for load in loads[4:7]:
        load.start()
    loads[0].wait()
    for load in loads[1:4]:
        load.start()
    lens_load = pltpu.make_async_copy(lens_hbm, lens_smem, w_sem.at[14])
    lens_load.start()
    st_col[...] = jnp.zeros_like(st_col)
    x = h_ref[...].astype(F32)
    ss_send[...] = column_to_row(jnp.sum(x * x, axis=-1, keepdims=True))
    wait_barrier()
    for i, peer in enumerate((nxt, prv, far)):
        go(ss_send, ss_recv.at[i], ss_s.at[i], ss_r.at[i], 'dm', peer)
    for load in loads[4:7]:
        load.wait()
    hd = cos_ref.shape[1]
    cos2[:, :hd] = cos_ref[...]
    cos2[:, hd:] = cos_ref[...]
    sin2[:, :hd] = -sin_ref[...]
    sin2[:, hd:] = sin_ref[...]
    for i, peer in enumerate((nxt, prv, far)):
        got(ss_recv.at[i], ss_s.at[i], ss_r.at[i], 'dm', peer)
    for load in loads[7:]:
        load.start()
    total = ss_send[...] + ss_recv[0] + ss_recv[1] + ss_recv[2]
    scale = row_to_column(lax.rsqrt(total / width_full + EPS))
    x_buf[...] = scale_rows(h_ref[...].astype(F32), scale, g1_ref[...].astype(F32)[None, :])

    def prow(owner, b, s):
        return pl.ds(al(owner * rows + b * rb + s * rh, rh), rh)

    def qkv_a(b, t):
        for d in range(2):
            go(part.at[t, prow(far, b, d)], a_recv.at[b, d, t], a_s.at[b, d, t], a_r.at[b, d, t], 'dm', ypeers[d])

    def qkv_b(b, t):
        for d in range(2):
            go(part.at[t, prow(ypeers[d], b, 1 - d)], b_recv.at[b, d, t], b_s.at[b, d, t], b_r.at[b, d, t], 'dm', ypeers[d])

    def qkv_c(b, t):
        for d in range(2):
            got(a_recv.at[b, d, t], a_s.at[b, d, t], a_r.at[b, d, t], 'dm', ypeers[d])
            c_send[b, d, t] = a_recv[b, d, t] + part[t, prow(ypeers[d], b, d)]
            go(c_send.at[b, d, t], c_recv.at[b, d, t], c_s.at[b, d, t], c_r.at[b, d, t], 'dm', ypeers[d])

    def totals(b):
        for t, out in enumerate((q_buf, k_out, v_out)):
            for d in range(2):
                got(b_recv.at[b, d, t], b_s.at[b, d, t], b_r.at[b, d, t], 'dm', ypeers[d])
                got(c_recv.at[b, d, t], c_s.at[b, d, t], c_r.at[b, d, t], 'dm', ypeers[d])
            for d in range(2):
                tot = part[t, prow(dm, b, d)] + c_recv[b, d, t] + b_recv[b, 1 - d, t]
                here = slice(b * rb + d * rh, b * rb + (d + 1) * rh)
                for i in range(heads):
                    y = tot[:, i * head:(i + 1) * head]
                    if t < 2:
                        y = y * cos2[here] + pltpu.roll(y, head // 2, 1) * sin2[here]
                    out[here, i * head:(i + 1) * head] = y.astype(BF16).astype(F32)

    span = heads * slots
    group = 8

    def attention(lo, hi):
        lane = lax.broadcasted_iota(jnp.int32, (8, span), 1)
        lane_slot = lane % slots
        own_head = (lane // slots) == lax.broadcasted_iota(jnp.int32, (8, span), 0)
        head_row = lax.broadcasted_iota(jnp.int32, (8, head), 0)

        def body(g, carry):
            first = al(g * group, group)
            vals = [ref[pl.ds(first, group), :] for ref in (q_buf, k_out, v_out)]

            def per_head(val, r):
                y = jnp.zeros((8, head), F32)
                for i in range(heads):
                    y = jnp.where(head_row == i, jnp.broadcast_to(val[r:r + 1, i * head:(i + 1) * head], (8, head)), y)
                return y

            scores, masks, news = [], [], []
            for r in range(group):
                q = per_head(vals[0], r)
                k = kc[first + r].reshape(span, head)
                s = lax.dot_general(q.astype(BF16), k, (((1,), (1,)), ((), ())), preferred_element_type=F32)
                masks.append(own_head & (lane_slot < lens_smem[first + r]))
                scores.append(jnp.where(masks[r], s * (head ** -0.5), float(jnp.finfo(F32).min)))
                news.append(jnp.sum(q * per_head(vals[1], r), axis=-1, keepdims=True) * (head ** -0.5))
            s, new = jnp.stack(scores), jnp.stack(news)
            top = jnp.maximum(jnp.max(s, axis=-1, keepdims=True), new)
            p = jnp.where(jnp.stack(masks), jnp.exp(s - top), 0.0)
            p_new = jnp.exp(new - top)
            den = jnp.sum(p, axis=-1, keepdims=True) + p_new
            p = (p / den).astype(BF16)
            p_new = (p_new / den).astype(BF16).astype(F32)
            for r in range(group):
                o = jnp.dot(p[r], vc[first + r].reshape(span, head), preferred_element_type=F32) + p_new[r] * per_head(vals[2], r)
                for i in range(heads):
                    o_own[g, r:r + 1, i * head:(i + 1) * head] = o[i:i + 1]
            return carry

        lax.fori_loop(lo, hi, body, 0)

    def orow(owner, s=0, n=rb):
        return pl.ds(al(owner * rb + s, 16), n)

    def o_send(b):
        o_all[b, orow(dm)] = o_own[b * rb // group:(b + 1) * rb // group].reshape(rb, heads * head).astype(BF16)
        mine = o_all.at[b, orow(dm)]
        for k, peer in enumerate(yall):
            go(mine, mine, o_s.at[b, k], o_r.at[b, k], 'dm', peer)

    def o_done(b):
        for k, peer in enumerate(yall):
            got(o_all.at[b, orow(yall[source[k]])], o_s.at[b, k], o_r.at[b, k], 'dm', peer)

    def trow(owner, c, s=0, n=share):
        return pl.ds(al(c * (brows // 2) + owner * share + s, sh), n)

    order = (xf, xn, xp, xi)

    def xs_pair(u, b):
        for i, owner in enumerate(order):
            go(full.at[u, b, trow(owner, 1 - core)], d2d_recv.at[u, b, i], d_s.at[u, b, i], d_r.at[u, b, i], 'tp', partner)

    def xs_ab(u, b):
        for i, owner in enumerate(order):
            got(d2d_recv.at[u, b, i], d_s.at[u, b, i], d_r.at[u, b, i], 'tp', partner)
            here = trow(owner, core)
            full[u, b, here] = full[u, b, here] + d2d_recv[u, b, i]
            if i < 3:
                go(full.at[u, b, here], xs_recv.at[u, b, i], xs_s.at[u, b, i], xs_r.at[u, b, i], 'tp', xids[i])

    def xs_done(u, b):
        for i in range(3):
            got(xs_recv.at[u, b, i], xs_s.at[u, b, i], xs_r.at[u, b, i], 'tp', xids[i])
        return (full[u, b, trow(xi, core)] + xs_recv[u, b, 0]) + (xs_recv[u, b, 1] + xs_recv[u, b, 2])

    def ag_send(u, buf, b):
        mine = buf.at[b, trow(xi, core)]
        for k in range(3):
            go(mine, mine, ag_s.at[u, b, k], ag_r.at[u, b, k], 'tp', xids[k])
        go(mine, mine, agd_s.at[u, b, 3], agd_r.at[u, b, 3], 'tp', partner)

    def ag_fwd(u, buf, b):
        for k in (1, 2, 0):
            came = buf.at[b, trow(xall[source[k]], core)]
            got(came, ag_s.at[u, b, k], ag_r.at[u, b, k], 'tp', xids[k])
            go(came, came, agd_s.at[u, b, k], agd_r.at[u, b, k], 'tp', partner)

    def ag_done(u, buf, b):
        for k in range(3):
            got(buf.at[b, trow(xall[source[k]], 1 - core)], agd_s.at[u, b, k], agd_r.at[u, b, k], 'tp', partner)
        got(buf.at[b, trow(xi, 1 - core)], agd_s.at[u, b, 3], agd_r.at[u, b, 3], 'tp', partner)

    step = 256

    def o_proj(b):
        o_done(b)
        need(9)
        for n in range(0, width, step):
            full[0, b, :, n:n + step] = jnp.dot(o_all[b], wo[:, n:n + step], preferred_element_type=F32)
        xs_pair(0, b)

    def norm_send(b):
        attn = xs_done(0, b)
        first = trow(xi, core).start
        owner = first // rb
        here = pl.ds(al(owner * rows + b * rb + (first - owner * rb), share), share)
        h1 = h_ref[here] + attn.astype(BF16)
        h1_all[b, trow(xi, core)] = h1
        ag_send(0, h1_all, b)
        h1 = h1.astype(F32)
        col = jnp.sum(h1 * h1, axis=-1, keepdims=True)
        st_col[b, trow(xi, core)] = jnp.broadcast_to(col, (share, 128))
        st_send[b] = st_col[b].T[:8]
        for k, peer in enumerate(yall):
            go(st_send.at[b], st_recv.at[b, k], st_s.at[b, k], st_r.at[b, k], 'dm', peer)

    def norm_mid(b):
        for k, peer in enumerate(yall):
            got(st_recv.at[b, k], st_s.at[b, k], st_r.at[b, k], 'dm', peer)
        sc_send[b] = st_send[b] + st_recv[b, 0] + st_recv[b, 1] + st_recv[b, 2]
        for i in range(2 * nx - 1):
            go(sc_send.at[b], sc_recv.at[b, i], sc_s.at[b, i], sc_r.at[b, i], 'tp', lax.rem(tp + i + 1, 2 * nx))

    def norm_done(b):
        total = sc_send[b]
        for i in range(2 * nx - 1):
            got(sc_recv.at[b, i], sc_s.at[b, i], sc_r.at[b, i], 'tp', lax.rem(tp + i + 1, 2 * nx))
            total = total + sc_recv[b, i]
        ag_done(0, h1_all, b)
        need(10)
        scale = row_to_column(lax.rsqrt(total / width_full + EPS))
        x2_all[b] = scale_rows(h1_all[b].astype(F32), scale, g2_ref[...].astype(F32)[None, :])

    def columns(owner):
        return pl.ds(al(owner * own_cols, 16), own_cols)

    def gu_part(b, i):
        need(11, 12)
        for j, w in enumerate((wg, wu)):
            y = lax.dot_general(w[columns((far, nxt, prv, dm)[i])], x2_all[b], (((1,), (1,)), ((), ())), preferred_element_type=F32)
            for p in range(PARTS):
                for s in range(2):
                    gu[b, i, p, s, j] = y[p * pc + s * ph:p * pc + (s + 1) * ph]
        for p in range(PARTS):
            if i == 0:
                for d in range(2):
                    go(gu.at[b, 0, p, d], ga_recv.at[b, d, p], ga_s.at[b, d, p], ga_r.at[b, d, p], 'dm', ypeers[d])
            elif i < 3:
                d = i - 1
                go(gu.at[b, i, p, 1 - d], gb_recv.at[b, d, p], gb_s.at[b, d, p], gb_r.at[b, d, p], 'dm', ypeers[d])

    def gu_c(b, p):
        for d in range(2):
            got(ga_recv.at[b, d, p], ga_s.at[b, d, p], ga_r.at[b, d, p], 'dm', ypeers[d])
            gc_send[b, d, p] = ga_recv[b, d, p] + gu[b, 1 + d, p, d]
            go(gc_send.at[b, d, p], gc_recv.at[b, d, p], gc_s.at[b, d, p], gc_r.at[b, d, p], 'dm', ypeers[d])

    cut = (pc // 2 + 15) // 16 * 16
    cuts = ((0, cut), (cut, pc - cut))

    def mrow(owner, p, s=0, n=pc):
        return pl.ds(al(owner * own_cols + p * pc + s, 16), n)

    def straight(b):
        return b == BATCHES - 1

    def m_send(b, p):
        for d in range(2):
            got(gb_recv.at[b, d, p], gb_s.at[b, d, p], gb_r.at[b, d, p], 'dm', ypeers[d])
            got(gc_recv.at[b, d, p], gc_s.at[b, d, p], gc_r.at[b, d, p], 'dm', ypeers[d])
        halves = []
        for d in range(2):
            gate, up = (gu[b, 3, p, d, j] + gc_recv[b, d, p, j] + gb_recv[b, 1 - d, p, j] for j in range(2))
            halves.append(gate * jax.nn.sigmoid(gate) * up)
        m_all[b, mrow(dm, p)] = jnp.concatenate(halves, axis=0).astype(BF16)
        mine = m_all.at[b, mrow(dm, p)]
        if straight(b):
            go(mine, mine, mf_s.at[b, 0, p], mf_r.at[b, 0, p], 'dm', far)
        for d in range(2):
            go(mine, mine, m_s.at[b, d, p], m_r.at[b, d, p], 'dm', ypeers[d])

    def m_fwd(b, p):
        for d in range(2):
            got(m_all.at[b, mrow(ypeers[1 - d], p)], m_s.at[b, d, p], m_r.at[b, d, p], 'dm', ypeers[d])
            if not straight(b):
                piece = m_all.at[b, mrow(ypeers[1 - d], p, *cuts[d])]
                go(piece, piece, mf_s.at[b, d, p], mf_r.at[b, d, p], 'dm', ypeers[d])

    def m_done(b):
        for p in range(PARTS):
            if straight(b):
                got(m_all.at[b, mrow(far, p)], mf_s.at[b, 0, p], mf_r.at[b, 0, p], 'dm', far)
            else:
                for d in range(2):
                    got(m_all.at[b, mrow(far, p, *cuts[d])], mf_s.at[b, d, p], mf_r.at[b, d, p], 'dm', ypeers[d])

    def down(b):
        m_done(b)
        need(13)
        for n in range(0, width, step):
            full[1, b, :, n:n + step] = lax.dot_general(m_all[b], wd[:, n:n + step], (((0,), (0,)), ((), ())), preferred_element_type=F32)
        xs_pair(1, b)

    def h_send(b):
        mlp = xs_done(1, b)
        h_all[b, trow(xi, core)] = h1_all[b, trow(xi, core)] + mlp.astype(BF16)
        ag_send(1, h_all, b)

    def h_done(b):
        ag_done(1, h_all, b)
        for owner in range(nd):
            out_ref[owner * rows + b * rb:owner * rows + (b + 1) * rb] = h_all[b, owner * rb:(owner + 1) * rb]

    waited = set()

    def need(*which):
        for i in which:
            if i not in waited:
                waited.add(i)
                loads[i].wait()

    def mm(t):
        need(1 + t)
        for i in range(heads):
            part[t, :, i * head:(i + 1) * head] = jnp.dot(x_buf[...], wqkv[t, i], preferred_element_type=F32)

    mm(0)
    qkv_a(0, 0)
    qkv_b(0, 0)
    mm(1)
    mm(2)
    qkv_a(0, 1)
    qkv_a(0, 2)
    qkv_a(1, 0)
    qkv_b(0, 2)
    qkv_b(0, 1)
    qkv_a(1, 1)
    qkv_c(0, 0)
    qkv_a(1, 2)
    qkv_c(0, 1)
    qkv_c(0, 2)
    qkv_c(1, 0)
    qkv_b(1, 0)
    qkv_c(1, 1)
    qkv_b(1, 2)
    qkv_c(1, 2)
    qkv_b(1, 1)
    totals(0)
    need(7, 8)
    lens_load.wait()
    attention(2, 4)
    attention(0, 2)
    o_send(0)
    totals(1)
    attention(6, 8)
    attention(4, 6)
    o_send(1)
    o_proj(0)
    xs_ab(0, 0)
    o_proj(1)
    xs_ab(0, 1)
    norm_send(0)
    norm_mid(0)
    norm_send(1)
    ag_fwd(0, h1_all, 0)
    norm_done(0)
    gu_part(0, 0)
    norm_mid(1)
    ag_fwd(0, h1_all, 1)
    gu_part(0, 1)
    norm_done(1)
    gu_part(1, 0)
    gu_part(0, 2)
    gu_part(0, 3)
    gu_c(0, 0)
    gu_c(0, 1)
    gu_c(0, 2)
    gu_part(1, 1)
    m_send(0, 0)
    m_send(0, 1)
    m_send(0, 2)
    gu_part(1, 2)
    gu_part(1, 3)
    gu_c(1, 1)
    gu_c(1, 2)
    gu_c(1, 0)
    m_fwd(0, 0)
    m_fwd(0, 1)
    m_fwd(0, 2)
    m_send(1, 1)
    m_send(1, 2)
    m_send(1, 0)
    down(0)
    m_fwd(1, 1)
    xs_ab(1, 0)
    m_fwd(1, 2)
    m_fwd(1, 0)
    down(1)
    xs_ab(1, 1)
    h_send(0)
    h_send(1)
    ag_fwd(1, h_all, 0)
    h_done(0)
    ag_fwd(1, h_all, 1)
    h_done(1)
    for copy in sends:
        copy.wait_send()


def layer(nd, nx, lens, hidden, g1, g2, cos, sin, wq, wk, wv, wo, wg, wu, wd, kc, vc):
    batch, width = hidden.shape
    heads, _, head = wq.shape
    rows, inner, cols = batch // nd, heads * head, wd.shape[0]
    nb = BATCHES
    rh = rows // nb // 2
    brows = batch // nb
    share = brows // (2 * nx)
    vmem = pl.BlockSpec(memory_space=pltpu.VMEM)
    hbm = pl.BlockSpec(memory_space=pl.ANY)
    vm = pltpu.VMEM
    dma = pltpu.SemaphoreType.DMA
    piece = vm((nb, 2, 3, rh, inner), F32)
    ph = cols // nd // PARTS // 2
    gpiece = vm((nb, 2, PARTS, 2, ph, brows), F32)
    return pl.pallas_call(
        functools.partial(layer_kernel, nd, nx, width * nd),
        out_shape=[vm((batch, width), BF16), vm((rows, inner), F32), vm((rows, inner), F32), vm(kc.shape, BF16), vm(vc.shape, BF16)],
        in_specs=[hbm] * 15,
        out_specs=[vmem] * 5,
        scratch_shapes=[
            pltpu.SMEM(lens.shape, jnp.int32), vm(hidden.shape, BF16), vm(g1.shape, BF16), vm(g2.shape, BF16), vm(cos.shape, F32), vm(sin.shape, F32),
            vm((3, heads, width, head), BF16), vm(wo.shape, BF16), vm(wg.shape, BF16), vm(wu.shape, BF16), vm(wd.shape, BF16),
            vm((batch, width), BF16), vm((3, batch, inner), F32), vm((8, batch), F32), vm((3, 8, batch), F32),
            piece, piece, piece, piece, vm((rows, head), F32), vm((rows, head), F32), vm((rows, inner), F32), vm((rows // 8, 8, inner), F32),
            vm((nb, brows, inner), BF16), vm((2, nb, brows, width), F32), vm((2, nb, nx, share, width), F32),
            vm((2, nb, 3, share, width), F32), vm((nb, brows, width), BF16), vm((nb, brows, 128), F32), vm((nb, 8, brows), F32), vm((nb, 3, 8, brows), F32),
            vm((nb, 8, brows), F32), vm((nb, 2 * nx - 1, 8, brows), F32), vm((nb, brows, width), BF16),
            vm((nb, 4, PARTS, 2, 2, ph, brows), F32), gpiece, gpiece, gpiece, gpiece, vm((nb, cols, brows), BF16), vm((nb, brows, width), BF16),
            dma((15,)), dma((3,)), dma((3,))] + [dma((nb, 2, 3))] * 6 + [dma((nb, 3))] * 2 + [dma((2, nb, nx))] * 2 + [dma((2, nb, 3))] * 2
        + [dma((nb, 3))] * 2 + [dma((nb, 2 * nx - 1))] * 2 + [dma((2, nb, 3))] * 2 + [dma((2, nb, nx))] * 2 + [dma((nb, 2, PARTS))] * 10,
        compiler_params=pltpu.CompilerParams(collective_id=0, has_side_effects=True, vmem_limit_bytes=LAYER_VMEM),
        name='layer',
    )(lens, hidden, g1, g2, cos, sin, wq, wk, wv, wo, wg, wu, wd, kc, vc)


def update_kernel(lens_ref, kn_ref, vn_ref, h_ref, kc, vc, ko_hbm, vo_hbm, out_hbm, k_win, v_win, bulk_sem, win_sem, h_sem):
    rows, heads, slots, head = kc.shape
    chunk = rows // UPDATE_CHUNKS
    window = k_win.shape[2]
    pos = lax.broadcasted_iota(jnp.int32, (heads, window, head), 1)
    sides = ((kn_ref, kc, k_win, ko_hbm), (vn_ref, vc, v_win, vo_hbm))

    def here(c):
        return pl.ds(pl.multiple_of(c * chunk, chunk), chunk)

    def bulk(i, c):
        return pltpu.make_async_copy(sides[i][1].at[here(c)], sides[i][3].at[here(c)], bulk_sem.at[i, c])

    for c in range(UPDATE_CHUNKS):
        for i in range(2):
            bulk(i, c).start()
    h_copy = pltpu.make_async_copy(h_ref, out_hbm, h_sem)
    h_copy.start()

    def base_of(row):
        return pl.multiple_of(lens_ref[row] // window * window, window)

    def patch(c, carry):
        first = pl.multiple_of(c * chunk, chunk)
        new_all = [side[0][pl.ds(first, chunk), :] for side in sides]
        for r in range(chunk):
            base = base_of(first + r)
            write = pos == lens_ref[first + r] - base
            for vals, (_, cache, win, _) in zip(new_all, sides):
                new = jnp.stack([jnp.broadcast_to(vals[r:r + 1, i * head:(i + 1) * head], (window, head)) for i in range(heads)])
                win[first + r] = jnp.where(write, new, cache[first + r, :, pl.ds(base, window), :].astype(F32)).astype(BF16)
        return carry

    lax.fori_loop(0, UPDATE_CHUNKS, patch, 0)

    def put(c, carry):
        for i, (_, _, win, out) in enumerate(sides):
            bulk(i, c).wait()
            for r in range(chunk):
                row = c * chunk + r
                pltpu.make_async_copy(win.at[row], out.at[row, :, pl.ds(base_of(row), window), :], win_sem.at[i, c]).start()
        return carry

    lax.fori_loop(0, UPDATE_CHUNKS, put, 0)
    for c in range(UPDATE_CHUNKS):
        for i, (_, _, win, out) in enumerate(sides):
            pltpu.make_async_copy(win.at[here(c)], out.at[here(c), :, pl.ds(0, window), :], win_sem.at[i, c]).wait()
    h_copy.wait()


def update(lens, kn, vn, h, kc, vc):
    rows, heads, slots, head = kc.shape
    window = 16
    smem = pl.BlockSpec(memory_space=pltpu.SMEM)
    vmem = pl.BlockSpec(memory_space=pltpu.VMEM)
    hbm = pl.BlockSpec(memory_space=pl.ANY)
    dma = pltpu.SemaphoreType.DMA
    return pl.pallas_call(
        update_kernel,
        in_specs=[smem] + [vmem] * 5,
        out_specs=[hbm] * 3,
        out_shape=[jax.ShapeDtypeStruct(kc.shape, BF16), jax.ShapeDtypeStruct(vc.shape, BF16), jax.ShapeDtypeStruct(h.shape, BF16)],
        scratch_shapes=[pltpu.VMEM((rows, heads, window, head), BF16), pltpu.VMEM((rows, heads, window, head), BF16),
                        dma((2, UPDATE_CHUNKS)), dma((2, UPDATE_CHUNKS)), dma],
        compiler_params=pltpu.CompilerParams(vmem_limit_bytes=UPDATE_VMEM),
        name='update',
    )(lens, *(pltpu.with_memory_space_constraint(x, pltpu.VMEM) for x in (kn, vn, h, kc, vc)))


def solution(mesh):
    nd, nx = mesh.shape['dm'], mesh.shape['tp'] // 2
    row_spec = P('dp', 'dm')
    cache_spec = P(('dp', 'dm'), None, 'tp', None)
    batch_spec = P(('dp', 'dm'))
    rope_spec = P(('dp', 'dm'), None)
    in_specs = (row_spec, P('dm', 'tp', None), P('dm', 'tp', None), P('dm', 'tp', None), P('tp', None, 'dm'), P('dm', 'tp'), P('dm', 'tp'), P('tp', 'dm'), P('dm'), P('dm'), cache_spec, cache_spec, batch_spec, rope_spec, rope_spec)
    out_specs = (row_spec, cache_spec, cache_spec)

    def local_layer(hidden, w_q, w_k, w_v, w_o, w_gate, w_up, w_down, norm_attn, norm_mlp, k_cache, v_cache, seq_lens, rope_cos, rope_sin):
        wq, wk, wv = (w.transpose(1, 0, 2) for w in (w_q, w_k, w_v))
        kc, vc = (c.transpose(0, 2, 1, 3) for c in (k_cache, v_cache))
        h_out, kn, vn, kc, vc = layer(nd, nx, seq_lens, hidden, norm_attn, norm_mlp, rope_cos, rope_sin, wq, wk, wv, w_o.reshape(-1, w_o.shape[-1]), w_gate.T, w_up.T, w_down, kc, vc)
        ko, vo, h_out = update(seq_lens, kn, vn, h_out, kc, vc)
        return h_out, ko.transpose(0, 2, 1, 3), vo.transpose(0, 2, 1, 3)

    return jax.shard_map(local_layer, mesh=mesh, in_specs=in_specs, out_specs=out_specs, check_vma=False)
```

```python
import functools

import jax
import jax.numpy as jnp
from jax import lax
from jax.experimental import pallas as pl
from jax.experimental.pallas import tpu as pltpu
from jax.sharding import PartitionSpec as P

EPS = 1e-6
F32 = jnp.float32
BF16 = jnp.bfloat16
MESH = pl.DeviceIdType.MESH
LAYER_VMEM = 52 * 2 ** 20
UPDATE_VMEM = 16 * 2 ** 20
BATCHES = 2
UPDATE_CHUNKS = 8
PARTS = 3


def remote(src, dst, send, recv, axis, index):
    return pltpu.make_async_remote_copy(
        src_ref=src, dst_ref=dst, send_sem=send, recv_sem=recv, device_id={axis: index}, device_id_type=MESH)


def entry_barrier(peers):
    barrier = pltpu.get_barrier_semaphore()
    for axis, index in peers:
        pl.semaphore_signal(barrier, inc=1, device_id={axis: index}, device_id_type=MESH)
    return lambda: pl.semaphore_wait(barrier, len(peers))


def column_to_row(col):
    rows = col.shape[0]
    return jnp.concatenate(
        [jnp.broadcast_to(col[i:i + 128], (128, 128)).T[:8] for i in range(0, rows, 128)], axis=1)


def row_to_column(row):
    rows = row.shape[1]
    return jnp.concatenate(
        [jnp.broadcast_to(row[:1, i:i + 128], (128, 128)).T for i in range(0, rows, 128)], axis=0)


def scale_rows(x, scale, gain):
    width = x.shape[1]
    cols = [x[:, i:i + 128] * scale * gain[:, i:i + 128] for i in range(0, width, 128)]
    return jnp.concatenate(cols, axis=1).astype(BF16)


def layer_kernel(nd, nx, width_full, lens_hbm, h_hbm, g1_hbm, g2_hbm, cos_hbm, sin_hbm, wq_hbm, wk_hbm, wv_hbm, wo_hbm, wg_hbm, wu_hbm, wd_hbm,
                 kc_hbm, vc_hbm, out_ref, k_out, v_out, kc, vc, lens_smem,
                 h_ref, g1_ref, g2_ref, cos_ref, sin_ref, wqkv, wo, wg, wu, wd,
                 x_buf, part, ss_send, ss_recv, a_recv, b_recv, c_send, c_recv, cos2, sin2, q_buf, o_own,
                 o_all, full, d2d_recv, xs_recv, h1_all, st_col, st_send, st_recv, sc_send, sc_recv, x2_all,
                 gu, ga_recv, gb_recv, gc_send, gc_recv, m_all, h_all,
                 w_sem, ss_s, ss_r, a_s, a_r, b_s, b_r, c_s, c_r, o_s, o_r, d_s, d_r, xs_s, xs_r,
                 st_s, st_r, sc_s, sc_r, ag_s, ag_r, agd_s, agd_r, ga_s, ga_r, gb_s, gb_r, gc_s, gc_r, m_s, m_r, mf_s, mf_r):
    dm, tp = lax.axis_index('dm'), lax.axis_index('tp')
    nxt, prv, far = lax.rem(dm + 1, nd), lax.rem(dm + nd - 1, nd), lax.rem(dm + 2, nd)
    core, xi = lax.rem(tp, 2), tp // 2
    xn, xp, xf = lax.rem(xi + 1, nx), lax.rem(xi + nx - 1, nx), lax.rem(xi + 2, nx)
    partner = tp + 1 - 2 * core
    ypeers, yall = (nxt, prv), (far, nxt, prv)
    xall = (xf, xn, xp)
    xids = tuple(2 * x + core for x in xall)
    source = (0, 2, 1)
    batch, width = h_ref.shape
    heads, slots, head = kc.shape[1:]
    rows = batch // nd
    rb = rows // BATCHES
    rh = rb // 2
    brows = nd * rb
    share = brows // (2 * nx)
    sh = share // 2
    cols = wd.shape[0]
    own_cols = cols // nd
    pc = own_cols // PARTS
    ph = pc // 2
    sends = []

    def go(*args):
        sends.append(remote(*args))
        sends[-1].start()

    def got(ref, send, recv, axis, index):
        remote(ref, ref, send, recv, axis, index).wait_recv()

    def al(x, n):
        return pl.multiple_of(x, n)

    wait_barrier = entry_barrier([('dm', y) for y in yall] + [('tp', lax.rem(tp + i, 2 * nx)) for i in range(1, 2 * nx)])
    pairs = ((h_hbm, h_ref), (wq_hbm, wqkv.at[0]), (wk_hbm, wqkv.at[1]), (wv_hbm, wqkv.at[2]), (g1_hbm, g1_ref), (cos_hbm, cos_ref), (sin_hbm, sin_ref),
             (kc_hbm, kc), (vc_hbm, vc), (wo_hbm, wo), (g2_hbm, g2_ref), (wg_hbm, wg), (wu_hbm, wu), (wd_hbm, wd))
    loads = [pltpu.make_async_copy(src, dst, w_sem.at[i]) for i, (src, dst) in enumerate(pairs)]
    loads[0].start()
    for load in loads[4:7]:
        load.start()
    loads[0].wait()
    for load in loads[1:4]:
        load.start()
    lens_load = pltpu.make_async_copy(lens_hbm, lens_smem, w_sem.at[14])
    lens_load.start()
    st_col[...] = jnp.zeros_like(st_col)
    x = h_ref[...].astype(F32)
    ss_send[...] = column_to_row(jnp.sum(x * x, axis=-1, keepdims=True))
    wait_barrier()
    for i, peer in enumerate((nxt, prv, far)):
        go(ss_send, ss_recv.at[i], ss_s.at[i], ss_r.at[i], 'dm', peer)
    for load in loads[4:7]:
        load.wait()
    hd = cos_ref.shape[1]
    cos2[:, :hd] = cos_ref[...]
    cos2[:, hd:] = cos_ref[...]
    sin2[:, :hd] = -sin_ref[...]
    sin2[:, hd:] = sin_ref[...]
    for i, peer in enumerate((nxt, prv, far)):
        got(ss_recv.at[i], ss_s.at[i], ss_r.at[i], 'dm', peer)
    for load in loads[7:]:
        load.start()
    total = ss_send[...] + ss_recv[0] + ss_recv[1] + ss_recv[2]
    scale = row_to_column(lax.rsqrt(total / width_full + EPS))
    x_buf[...] = scale_rows(h_ref[...].astype(F32), scale, g1_ref[...].astype(F32)[None, :])

    def prow(owner, b, s):
        return pl.ds(al(owner * rows + b * rb + s * rh, rh), rh)

    def qkv_a(b, t):
        for d in range(2):
            go(part.at[t, prow(far, b, d)], a_recv.at[b, d, t], a_s.at[b, d, t], a_r.at[b, d, t], 'dm', ypeers[d])

    def qkv_b(b, t):
        for d in range(2):
            go(part.at[t, prow(ypeers[d], b, 1 - d)], b_recv.at[b, d, t], b_s.at[b, d, t], b_r.at[b, d, t], 'dm', ypeers[d])

    def qkv_c(b, t):
        for d in range(2):
            got(a_recv.at[b, d, t], a_s.at[b, d, t], a_r.at[b, d, t], 'dm', ypeers[d])
            c_send[b, d, t] = a_recv[b, d, t] + part[t, prow(ypeers[d], b, d)]
            go(c_send.at[b, d, t], c_recv.at[b, d, t], c_s.at[b, d, t], c_r.at[b, d, t], 'dm', ypeers[d])

    def totals(b):
        for t, out in enumerate((q_buf, k_out, v_out)):
            for d in range(2):
                got(b_recv.at[b, d, t], b_s.at[b, d, t], b_r.at[b, d, t], 'dm', ypeers[d])
                got(c_recv.at[b, d, t], c_s.at[b, d, t], c_r.at[b, d, t], 'dm', ypeers[d])
            for d in range(2):
                tot = part[t, prow(dm, b, d)] + c_recv[b, d, t] + b_recv[b, 1 - d, t]
                here = slice(b * rb + d * rh, b * rb + (d + 1) * rh)
                for i in range(heads):
                    y = tot[:, i * head:(i + 1) * head]
                    if t < 2:
                        y = y * cos2[here] + pltpu.roll(y, head // 2, 1) * sin2[here]
                    out[here, i * head:(i + 1) * head] = y.astype(BF16).astype(F32)

    span = heads * slots
    group = 8

    def attention(lo, hi):
        lane = lax.broadcasted_iota(jnp.int32, (8, span), 1)
        lane_slot = lane % slots
        own_head = (lane // slots) == lax.broadcasted_iota(jnp.int32, (8, span), 0)
        head_row = lax.broadcasted_iota(jnp.int32, (8, head), 0)

        def body(g, carry):
            first = al(g * group, group)
            vals = [ref[pl.ds(first, group), :] for ref in (q_buf, k_out, v_out)]

            def per_head(val, r):
                y = jnp.zeros((8, head), F32)
                for i in range(heads):
                    y = jnp.where(head_row == i, jnp.broadcast_to(val[r:r + 1, i * head:(i + 1) * head], (8, head)), y)
                return y

            scores, masks, news = [], [], []
            for r in range(group):
                q = per_head(vals[0], r)
                k = kc[first + r].reshape(span, head)
                s = lax.dot_general(q.astype(BF16), k, (((1,), (1,)), ((), ())), preferred_element_type=F32)
                masks.append(own_head & (lane_slot < lens_smem[first + r]))
                scores.append(jnp.where(masks[r], s * (head ** -0.5), float(jnp.finfo(F32).min)))
                news.append(jnp.sum(q * per_head(vals[1], r), axis=-1, keepdims=True) * (head ** -0.5))
            s, new = jnp.stack(scores), jnp.stack(news)
            top = jnp.maximum(jnp.max(s, axis=-1, keepdims=True), new)
            p = jnp.where(jnp.stack(masks), jnp.exp(s - top), 0.0)
            p_new = jnp.exp(new - top)
            den = jnp.sum(p, axis=-1, keepdims=True) + p_new
            p = (p / den).astype(BF16)
            p_new = (p_new / den).astype(BF16).astype(F32)
            for r in range(group):
                o = jnp.dot(p[r], vc[first + r].reshape(span, head), preferred_element_type=F32) + p_new[r] * per_head(vals[2], r)
                for i in range(heads):
                    o_own[g, r:r + 1, i * head:(i + 1) * head] = o[i:i + 1]
            return carry

        lax.fori_loop(lo, hi, body, 0)

    def orow(owner, s=0, n=rb):
        return pl.ds(al(owner * rb + s, 16), n)

    def o_send(b):
        o_all[b, orow(dm)] = o_own[b * rb // group:(b + 1) * rb // group].reshape(rb, heads * head).astype(BF16)
        mine = o_all.at[b, orow(dm)]
        for k, peer in enumerate(yall):
            go(mine, mine, o_s.at[b, k], o_r.at[b, k], 'dm', peer)

    def o_done(b):
        for k, peer in enumerate(yall):
            got(o_all.at[b, orow(yall[source[k]])], o_s.at[b, k], o_r.at[b, k], 'dm', peer)

    def trow(owner, c, s=0, n=share):
        return pl.ds(al(c * (brows // 2) + owner * share + s, sh), n)

    order = (xf, xn, xp, xi)

    def xs_pair(u, b):
        for i, owner in enumerate(order):
            go(full.at[u, b, trow(owner, 1 - core)], d2d_recv.at[u, b, i], d_s.at[u, b, i], d_r.at[u, b, i], 'tp', partner)

    def xs_ab(u, b):
        for i, owner in enumerate(order):
            got(d2d_recv.at[u, b, i], d_s.at[u, b, i], d_r.at[u, b, i], 'tp', partner)
            here = trow(owner, core)
            full[u, b, here] = full[u, b, here] + d2d_recv[u, b, i]
            if i < 3:
                go(full.at[u, b, here], xs_recv.at[u, b, i], xs_s.at[u, b, i], xs_r.at[u, b, i], 'tp', xids[i])

    def xs_done(u, b):
        for i in range(3):
            got(xs_recv.at[u, b, i], xs_s.at[u, b, i], xs_r.at[u, b, i], 'tp', xids[i])
        return (full[u, b, trow(xi, core)] + xs_recv[u, b, 0]) + (xs_recv[u, b, 1] + xs_recv[u, b, 2])

    def ag_send(u, buf, b):
        mine = buf.at[b, trow(xi, core)]
        for k in range(3):
            go(mine, mine, ag_s.at[u, b, k], ag_r.at[u, b, k], 'tp', xids[k])
        go(mine, mine, agd_s.at[u, b, 3], agd_r.at[u, b, 3], 'tp', partner)

    def ag_fwd(u, buf, b):
        for k in (1, 2, 0):
            came = buf.at[b, trow(xall[source[k]], core)]
            got(came, ag_s.at[u, b, k], ag_r.at[u, b, k], 'tp', xids[k])
            go(came, came, agd_s.at[u, b, k], agd_r.at[u, b, k], 'tp', partner)

    def ag_done(u, buf, b):
        for k in range(3):
            got(buf.at[b, trow(xall[source[k]], 1 - core)], agd_s.at[u, b, k], agd_r.at[u, b, k], 'tp', partner)
        got(buf.at[b, trow(xi, 1 - core)], agd_s.at[u, b, 3], agd_r.at[u, b, 3], 'tp', partner)

    step = 256

    def o_proj(b):
        o_done(b)
        need(9)
        for n in range(0, width, step):
            full[0, b, :, n:n + step] = jnp.dot(o_all[b], wo[:, n:n + step], preferred_element_type=F32)
        xs_pair(0, b)

    def norm_send(b):
        attn = xs_done(0, b)
        first = trow(xi, core).start
        owner = first // rb
        here = pl.ds(al(owner * rows + b * rb + (first - owner * rb), share), share)
        h1 = h_ref[here] + attn.astype(BF16)
        h1_all[b, trow(xi, core)] = h1
        ag_send(0, h1_all, b)
        h1 = h1.astype(F32)
        col = jnp.sum(h1 * h1, axis=-1, keepdims=True)
        st_col[b, trow(xi, core)] = jnp.broadcast_to(col, (share, 128))
        st_send[b] = st_col[b].T[:8]
        for k, peer in enumerate(yall):
            go(st_send.at[b], st_recv.at[b, k], st_s.at[b, k], st_r.at[b, k], 'dm', peer)

    def norm_mid(b):
        for k, peer in enumerate(yall):
            got(st_recv.at[b, k], st_s.at[b, k], st_r.at[b, k], 'dm', peer)
        sc_send[b] = st_send[b] + st_recv[b, 0] + st_recv[b, 1] + st_recv[b, 2]
        for i in range(2 * nx - 1):
            go(sc_send.at[b], sc_recv.at[b, i], sc_s.at[b, i], sc_r.at[b, i], 'tp', lax.rem(tp + i + 1, 2 * nx))

    def norm_done(b):
        total = sc_send[b]
        for i in range(2 * nx - 1):
            got(sc_recv.at[b, i], sc_s.at[b, i], sc_r.at[b, i], 'tp', lax.rem(tp + i + 1, 2 * nx))
            total = total + sc_recv[b, i]
        ag_done(0, h1_all, b)
        need(10)
        scale = row_to_column(lax.rsqrt(total / width_full + EPS))
        x2_all[b] = scale_rows(h1_all[b].astype(F32), scale, g2_ref[...].astype(F32)[None, :])

    def columns(owner):
        return pl.ds(al(owner * own_cols, 16), own_cols)

    def gu_part(b, i):
        need(11, 12)
        for j, w in enumerate((wg, wu)):
            y = lax.dot_general(w[columns((far, nxt, prv, dm)[i])], x2_all[b], (((1,), (1,)), ((), ())), preferred_element_type=F32)
            for p in range(PARTS):
                for s in range(2):
                    gu[b, i, p, s, j] = y[p * pc + s * ph:p * pc + (s + 1) * ph]
        for p in range(PARTS):
            if i == 0:
                for d in range(2):
                    go(gu.at[b, 0, p, d], ga_recv.at[b, d, p], ga_s.at[b, d, p], ga_r.at[b, d, p], 'dm', ypeers[d])
            elif i < 3:
                d = i - 1
                go(gu.at[b, i, p, 1 - d], gb_recv.at[b, d, p], gb_s.at[b, d, p], gb_r.at[b, d, p], 'dm', ypeers[d])

    def gu_c(b, p):
        for d in range(2):
            got(ga_recv.at[b, d, p], ga_s.at[b, d, p], ga_r.at[b, d, p], 'dm', ypeers[d])
            gc_send[b, d, p] = ga_recv[b, d, p] + gu[b, 1 + d, p, d]
            go(gc_send.at[b, d, p], gc_recv.at[b, d, p], gc_s.at[b, d, p], gc_r.at[b, d, p], 'dm', ypeers[d])

    cut = (pc // 2 + 15) // 16 * 16
    cuts = ((0, cut), (cut, pc - cut))

    def mrow(owner, p, s=0, n=pc):
        return pl.ds(al(owner * own_cols + p * pc + s, 16), n)

    def straight(b):
        return b == BATCHES - 1

    def m_send(b, p):
        for d in range(2):
            got(gb_recv.at[b, d, p], gb_s.at[b, d, p], gb_r.at[b, d, p], 'dm', ypeers[d])
            got(gc_recv.at[b, d, p], gc_s.at[b, d, p], gc_r.at[b, d, p], 'dm', ypeers[d])
        halves = []
        for d in range(2):
            gate, up = (gu[b, 3, p, d, j] + gc_recv[b, d, p, j] + gb_recv[b, 1 - d, p, j] for j in range(2))
            halves.append(gate * jax.nn.sigmoid(gate) * up)
        m_all[b, mrow(dm, p)] = jnp.concatenate(halves, axis=0).astype(BF16)
        mine = m_all.at[b, mrow(dm, p)]
        if straight(b):
            go(mine, mine, mf_s.at[b, 0, p], mf_r.at[b, 0, p], 'dm', far)
        for d in range(2):
            go(mine, mine, m_s.at[b, d, p], m_r.at[b, d, p], 'dm', ypeers[d])

    def m_fwd(b, p):
        for d in range(2):
            got(m_all.at[b, mrow(ypeers[1 - d], p)], m_s.at[b, d, p], m_r.at[b, d, p], 'dm', ypeers[d])
            if not straight(b):
                piece = m_all.at[b, mrow(ypeers[1 - d], p, *cuts[d])]
                go(piece, piece, mf_s.at[b, d, p], mf_r.at[b, d, p], 'dm', ypeers[d])

    def m_done(b):
        for p in range(PARTS):
            if straight(b):
                got(m_all.at[b, mrow(far, p)], mf_s.at[b, 0, p], mf_r.at[b, 0, p], 'dm', far)
            else:
                for d in range(2):
                    got(m_all.at[b, mrow(far, p, *cuts[d])], mf_s.at[b, d, p], mf_r.at[b, d, p], 'dm', ypeers[d])

    def down(b):
        m_done(b)
        need(13)
        for n in range(0, width, step):
            full[1, b, :, n:n + step] = lax.dot_general(m_all[b], wd[:, n:n + step], (((0,), (0,)), ((), ())), preferred_element_type=F32)
        xs_pair(1, b)

    def h_send(b):
        mlp = xs_done(1, b)
        h_all[b, trow(xi, core)] = h1_all[b, trow(xi, core)] + mlp.astype(BF16)
        ag_send(1, h_all, b)

    def h_done(b):
        ag_done(1, h_all, b)
        for owner in range(nd):
            out_ref[owner * rows + b * rb:owner * rows + (b + 1) * rb] = h_all[b, owner * rb:(owner + 1) * rb]

    waited = set()

    def need(*which):
        for i in which:
            if i not in waited:
                waited.add(i)
                loads[i].wait()

    def mm(t):
        need(1 + t)
        for i in range(heads):
            part[t, :, i * head:(i + 1) * head] = jnp.dot(x_buf[...], wqkv[t, i], preferred_element_type=F32)

    mm(0)
    qkv_a(0, 0)
    qkv_b(0, 0)
    mm(1)
    qkv_a(0, 1)
    mm(2)
    qkv_a(0, 2)
    qkv_b(0, 1)
    qkv_b(0, 2)
    qkv_c(0, 0)
    qkv_c(0, 1)
    qkv_c(0, 2)
    qkv_a(1, 0)
    qkv_a(1, 1)
    qkv_b(1, 1)
    totals(0)
    qkv_a(1, 2)
    qkv_b(1, 2)
    need(7, 8)
    lens_load.wait()
    attention(0, 2)
    attention(2, 4)
    o_send(0)
    qkv_b(1, 0)
    qkv_c(1, 0)
    qkv_c(1, 1)
    o_proj(0)
    qkv_c(1, 2)
    xs_ab(0, 0)
    totals(1)
    attention(4, 6)
    attention(6, 8)
    o_send(1)
    norm_send(0)
    norm_mid(0)
    o_proj(1)
    xs_ab(0, 1)
    ag_fwd(0, h1_all, 0)
    norm_done(0)
    gu_part(0, 0)
    norm_send(1)
    gu_part(0, 1)
    gu_part(0, 2)
    gu_part(0, 3)
    ag_fwd(0, h1_all, 1)
    norm_mid(1)
    gu_c(0, 1)
    gu_c(0, 2)
    gu_c(0, 0)
    norm_done(1)
    gu_part(1, 0)
    m_send(0, 1)
    m_send(0, 0)
    gu_part(1, 1)
    gu_part(1, 2)
    gu_c(1, 0)
    m_fwd(0, 0)
    m_send(0, 2)
    gu_c(1, 1)
    m_fwd(0, 1)
    gu_part(1, 3)
    gu_c(1, 2)
    m_fwd(0, 2)
    m_send(1, 0)
    m_send(1, 1)
    m_fwd(1, 1)
    m_send(1, 2)
    down(0)
    m_fwd(1, 2)
    xs_ab(1, 0)
    m_fwd(1, 0)
    down(1)
    xs_ab(1, 1)
    h_send(0)
    h_send(1)
    ag_fwd(1, h_all, 0)
    ag_fwd(1, h_all, 1)
    h_done(0)
    h_done(1)
    for copy in sends:
        copy.wait_send()


def layer(nd, nx, lens, hidden, g1, g2, cos, sin, wq, wk, wv, wo, wg, wu, wd, kc, vc):
    batch, width = hidden.shape
    heads, _, head = wq.shape
    rows, inner, cols = batch // nd, heads * head, wd.shape[0]
    nb = BATCHES
    rh = rows // nb // 2
    brows = batch // nb
    share = brows // (2 * nx)
    vmem = pl.BlockSpec(memory_space=pltpu.VMEM)
    hbm = pl.BlockSpec(memory_space=pl.ANY)
    vm = pltpu.VMEM
    dma = pltpu.SemaphoreType.DMA
    piece = vm((nb, 2, 3, rh, inner), F32)
    ph = cols // nd // PARTS // 2
    gpiece = vm((nb, 2, PARTS, 2, ph, brows), F32)
    return pl.pallas_call(
        functools.partial(layer_kernel, nd, nx, width * nd),
        out_shape=[vm((batch, width), BF16), vm((rows, inner), F32), vm((rows, inner), F32), vm(kc.shape, BF16), vm(vc.shape, BF16)],
        in_specs=[hbm] * 15,
        out_specs=[vmem] * 5,
        scratch_shapes=[
            pltpu.SMEM(lens.shape, jnp.int32), vm(hidden.shape, BF16), vm(g1.shape, BF16), vm(g2.shape, BF16), vm(cos.shape, F32), vm(sin.shape, F32),
            vm((3, heads, width, head), BF16), vm(wo.shape, BF16), vm(wg.shape, BF16), vm(wu.shape, BF16), vm(wd.shape, BF16),
            vm((batch, width), BF16), vm((3, batch, inner), F32), vm((8, batch), F32), vm((3, 8, batch), F32),
            piece, piece, piece, piece, vm((rows, head), F32), vm((rows, head), F32), vm((rows, inner), F32), vm((rows // 8, 8, inner), F32),
            vm((nb, brows, inner), BF16), vm((2, nb, brows, width), F32), vm((2, nb, nx, share, width), F32),
            vm((2, nb, 3, share, width), F32), vm((nb, brows, width), BF16), vm((nb, brows, 128), F32), vm((nb, 8, brows), F32), vm((nb, 3, 8, brows), F32),
            vm((nb, 8, brows), F32), vm((nb, 2 * nx - 1, 8, brows), F32), vm((nb, brows, width), BF16),
            vm((nb, 4, PARTS, 2, 2, ph, brows), F32), gpiece, gpiece, gpiece, gpiece, vm((nb, cols, brows), BF16), vm((nb, brows, width), BF16),
            dma((15,)), dma((3,)), dma((3,))] + [dma((nb, 2, 3))] * 6 + [dma((nb, 3))] * 2 + [dma((2, nb, nx))] * 2 + [dma((2, nb, 3))] * 2
        + [dma((nb, 3))] * 2 + [dma((nb, 2 * nx - 1))] * 2 + [dma((2, nb, 3))] * 2 + [dma((2, nb, nx))] * 2 + [dma((nb, 2, PARTS))] * 10,
        compiler_params=pltpu.CompilerParams(collective_id=0, has_side_effects=True, vmem_limit_bytes=LAYER_VMEM),
        name='layer',
    )(lens, hidden, g1, g2, cos, sin, wq, wk, wv, wo, wg, wu, wd, kc, vc)


def update_kernel(lens_ref, kn_ref, vn_ref, h_ref, kc, vc, ko_hbm, vo_hbm, out_hbm, k_win, v_win, bulk_sem, win_sem, h_sem):
    rows, heads, slots, head = kc.shape
    chunk = rows // UPDATE_CHUNKS
    window = k_win.shape[2]
    pos = lax.broadcasted_iota(jnp.int32, (heads, window, head), 1)
    sides = ((kn_ref, kc, k_win, ko_hbm), (vn_ref, vc, v_win, vo_hbm))

    def here(c):
        return pl.ds(pl.multiple_of(c * chunk, chunk), chunk)

    def bulk(i, c):
        return pltpu.make_async_copy(sides[i][1].at[here(c)], sides[i][3].at[here(c)], bulk_sem.at[i, c])

    for c in range(UPDATE_CHUNKS):
        for i in range(2):
            bulk(i, c).start()
    h_copy = pltpu.make_async_copy(h_ref, out_hbm, h_sem)
    h_copy.start()

    def base_of(row):
        return pl.multiple_of(lens_ref[row] // window * window, window)

    def patch(c, carry):
        first = pl.multiple_of(c * chunk, chunk)
        new_all = [side[0][pl.ds(first, chunk), :] for side in sides]
        for r in range(chunk):
            base = base_of(first + r)
            write = pos == lens_ref[first + r] - base
            for vals, (_, cache, win, _) in zip(new_all, sides):
                new = jnp.stack([jnp.broadcast_to(vals[r:r + 1, i * head:(i + 1) * head], (window, head)) for i in range(heads)])
                win[first + r] = jnp.where(write, new, cache[first + r, :, pl.ds(base, window), :].astype(F32)).astype(BF16)
        return carry

    lax.fori_loop(0, UPDATE_CHUNKS, patch, 0)

    def put(c, carry):
        for i, (_, _, win, out) in enumerate(sides):
            bulk(i, c).wait()
            for r in range(chunk):
                row = c * chunk + r
                pltpu.make_async_copy(win.at[row], out.at[row, :, pl.ds(base_of(row), window), :], win_sem.at[i, c]).start()
        return carry

    lax.fori_loop(0, UPDATE_CHUNKS, put, 0)
    for c in range(UPDATE_CHUNKS):
        for i, (_, _, win, out) in enumerate(sides):
            pltpu.make_async_copy(win.at[here(c)], out.at[here(c), :, pl.ds(0, window), :], win_sem.at[i, c]).wait()
    h_copy.wait()


def update(lens, kn, vn, h, kc, vc):
    rows, heads, slots, head = kc.shape
    window = 16
    smem = pl.BlockSpec(memory_space=pltpu.SMEM)
    vmem = pl.BlockSpec(memory_space=pltpu.VMEM)
    hbm = pl.BlockSpec(memory_space=pl.ANY)
    dma = pltpu.SemaphoreType.DMA
    return pl.pallas_call(
        update_kernel,
        in_specs=[smem] + [vmem] * 5,
        out_specs=[hbm] * 3,
        out_shape=[jax.ShapeDtypeStruct(kc.shape, BF16), jax.ShapeDtypeStruct(vc.shape, BF16), jax.ShapeDtypeStruct(h.shape, BF16)],
        scratch_shapes=[pltpu.VMEM((rows, heads, window, head), BF16), pltpu.VMEM((rows, heads, window, head), BF16),
                        dma((2, UPDATE_CHUNKS)), dma((2, UPDATE_CHUNKS)), dma],
        compiler_params=pltpu.CompilerParams(vmem_limit_bytes=UPDATE_VMEM),
        name='update',
    )(lens, *(pltpu.with_memory_space_constraint(x, pltpu.VMEM) for x in (kn, vn, h, kc, vc)))


def solution(mesh):
    nd, nx = mesh.shape['dm'], mesh.shape['tp'] // 2
    row_spec = P('dp', 'dm')
    cache_spec = P(('dp', 'dm'), None, 'tp', None)
    batch_spec = P(('dp', 'dm'))
    rope_spec = P(('dp', 'dm'), None)
    in_specs = (row_spec, P('dm', 'tp', None), P('dm', 'tp', None), P('dm', 'tp', None), P('tp', None, 'dm'), P('dm', 'tp'), P('dm', 'tp'), P('tp', 'dm'), P('dm'), P('dm'), cache_spec, cache_spec, batch_spec, rope_spec, rope_spec)
    out_specs = (row_spec, cache_spec, cache_spec)

    def local_layer(hidden, w_q, w_k, w_v, w_o, w_gate, w_up, w_down, norm_attn, norm_mlp, k_cache, v_cache, seq_lens, rope_cos, rope_sin):
        wq, wk, wv = (w.transpose(1, 0, 2) for w in (w_q, w_k, w_v))
        kc, vc = (c.transpose(0, 2, 1, 3) for c in (k_cache, v_cache))
        h_out, kn, vn, kc, vc = layer(nd, nx, seq_lens, hidden, norm_attn, norm_mlp, rope_cos, rope_sin, wq, wk, wv, w_o.reshape(-1, w_o.shape[-1]), w_gate.T, w_up.T, w_down, kc, vc)
        ko, vo, h_out = update(seq_lens, kn, vn, h_out, kc, vc)
        return h_out, ko.transpose(0, 2, 1, 3), vo.transpose(0, 2, 1, 3)

    return jax.shard_map(local_layer, mesh=mesh, in_specs=in_specs, out_specs=out_specs, check_vma=False)
```
